128 devices in a mesh: inner: 16 (over z, y), fsdp: 8 (over x, core).
Axes of the slice: x: 4, y: 4, z: 4, core: 2. Of those that a mesh axis runs over, the one named last changes fastest.
Arguments:
- x_in: bfloat16 [65536, 1024], P(('inner', 'fsdp'))
- w_up: bfloat16 [3, 1024, 4096], P(None, ('inner', 'fsdp'))
- w_down: bfloat16 [3, 4096, 1024], P(None, ('inner', 'fsdp'))
- grad_out: bfloat16 [65536, 1024], P(('inner', 'fsdp'))
Outputs:
- output 1: bfloat16 [65536, 1024], P(('inner', 'fsdp'))
- output 2: bfloat16 [65536, 1024], P(('inner', 'fsdp'))
- output 3: float32 [3, 1024, 4096], P(None, ('inner', 'fsdp'))
- output 4: float32 [3, 4096, 1024], P(None, ('inner', 'fsdp'))
All inputs are finite; a program needn't handle non-finite values.
Results may differ from the reference program's by a relative error of at most 0.00768654.
Values are sent between devices in bfloat16 or wider.
A program may use at most 1 GiB of HBM per device.

```python
import jax
import jax.numpy as jnp
from jax import lax

TOKENS = 65536
ROW_BLOCK = 512
D_MODEL = 1024
D_FF = 4096
LAYERS = 3


def gelu_parts(pre_act):
    norm_cdf = 0.5 * (1.0 + lax.erf(pre_act * (2.0 ** -0.5)))
    norm_pdf = jnp.exp(-0.5 * pre_act * pre_act) * ((2.0 * jnp.pi) ** -0.5)
    return pre_act * norm_cdf, norm_cdf + pre_act * norm_pdf


def setup_inputs(seed: int = 0) -> dict:
    base_key = jax.random.key(seed)
    key_x, key_up, key_down, key_g = jax.random.split(base_key, 4)
    x_in = jax.random.normal(key_x, (TOKENS, D_MODEL), jnp.float32).astype(jnp.bfloat16)
    w_up = (jax.random.normal(key_up, (LAYERS, D_MODEL, D_FF), jnp.float32) * D_MODEL ** -0.5).astype(jnp.bfloat16)
    w_down = (jax.random.normal(key_down, (LAYERS, D_FF, D_MODEL), jnp.float32) * D_FF ** -0.5).astype(jnp.bfloat16)
    grad_out = jax.random.normal(key_g, (TOKENS, D_MODEL), jnp.float32).astype(jnp.bfloat16)
    return {"x_in": x_in, "w_up": w_up, "w_down": w_down, "grad_out": grad_out}


def block_pass(x_blk, g_blk, w_up, w_down):
    def fwd_step(x_cur, weights):
        up_mat, down_mat = weights
        pre_act = jnp.dot(x_cur, up_mat, preferred_element_type=jnp.float32)
        post_act = gelu_parts(pre_act)[0].astype(jnp.bfloat16)
        branch = jnp.dot(post_act, down_mat, preferred_element_type=jnp.float32)
        return (x_cur.astype(jnp.float32) + branch).astype(jnp.bfloat16), x_cur

    y_blk, layer_inputs = lax.scan(fwd_step, x_blk, (w_up, w_down))

    def bwd_step(g_cur, scan_in):
        x_cur, up_mat, down_mat = scan_in
        pre_act = jnp.dot(x_cur, up_mat, preferred_element_type=jnp.float32)
        post_full, gelu_slope = gelu_parts(pre_act)
        post_act = post_full.astype(jnp.bfloat16)
        d_act = jnp.dot(g_cur, down_mat.T, preferred_element_type=jnp.float32)
        d_pre = (d_act * gelu_slope).astype(jnp.bfloat16)
        back_term = jnp.dot(d_pre, up_mat.T, preferred_element_type=jnp.float32)
        g_next = (g_cur.astype(jnp.float32) + back_term).astype(jnp.bfloat16)
        grad_up = jnp.dot(x_cur.T, d_pre, preferred_element_type=jnp.float32)
        grad_down = jnp.dot(post_act.T, g_cur, preferred_element_type=jnp.float32)
        return g_next, (grad_up, grad_down)

    g_in, layer_grads = lax.scan(bwd_step, g_blk, (layer_inputs, w_up, w_down), reverse=True)
    return y_blk, g_in, layer_grads[0], layer_grads[1]


def reference(x_in, w_up, w_down, grad_out):
    blocks = TOKENS // ROW_BLOCK
    x_blocks = x_in.reshape(blocks, ROW_BLOCK, D_MODEL)
    g_blocks = grad_out.reshape(blocks, ROW_BLOCK, D_MODEL)

    def block_step(running, scan_in):
        y_blk, g_in, grad_up, grad_down = block_pass(scan_in[0], scan_in[1], w_up, w_down)
        return (running[0] + grad_up, running[1] + grad_down), (y_blk, g_in)

    zero_sums = (jnp.zeros((LAYERS, D_MODEL, D_FF), jnp.float32), jnp.zeros((LAYERS, D_FF, D_MODEL), jnp.float32))
    grad_sums, per_block = lax.scan(block_step, zero_sums, (x_blocks, g_blocks))
    y_out = per_block[0].reshape(TOKENS, D_MODEL)
    grad_in = per_block[1].reshape(TOKENS, D_MODEL)
    return (y_out, grad_in, grad_sums[0], grad_sums[1])
```

```python
import functools

import jax
import jax.numpy as jnp
from jax import lax
from jax.experimental import pallas as pl
from jax.experimental.pallas import tpu as pltpu
from jax.sharding import Mesh, PartitionSpec as P

CHIPS = ("z", "y", "x")
ALL = CHIPS + ("c",)
BF16 = jnp.bfloat16
F32 = jnp.float32
SIDE = 4
ROWS = 16
ORDERS = (("x", "y", "z"), ("y", "z", "x"), ("z", "x", "y"))


def gelu_parts(pre_act):
    norm_cdf = 0.5 * (1.0 + lax.erf(pre_act * (2.0 ** -0.5)))
    norm_pdf = jnp.exp(-0.5 * pre_act * pre_act) * ((2.0 * jnp.pi) ** -0.5)
    return pre_act * norm_cdf, norm_cdf + pre_act * norm_pdf


def swap(val):
    return lax.ppermute(val, "c", [(0, 1), (1, 0)])


def pair_rows(own, core):
    got = swap(own)
    return jnp.where(core == 0, jnp.concatenate([own, got], 0), jnp.concatenate([got, own], 0))


def dot(eq, left, right):
    return jnp.einsum(eq, left, right, preferred_element_type=F32)


def jobs_of(width):
    tile = width // 8
    cuts = ((0, 3 * tile), (3 * tile, 3 * tile), (6 * tile, 2 * tile))
    whole = [(mat, (0, width), ORDERS[mat]) for mat in range(3)]
    return whole + [(3, cuts[k], ORDERS[k]) for k in range(3)]


def view(ref, lead, axes, sel, cols=None):
    mid = tuple(sel.get(a, slice(None)) for a in axes)
    last = (slice(None), pl.ds(*cols)) if cols is not None else ()
    return ref.at[lead + mid + last]


def half(axis, k):
    return {axis: pl.ds(2 * k, 2)}


def ring_places():
    me = {a: lax.axis_index(a) for a in CHIPS}
    near = {a: [lax.rem(me[a] + d, SIDE) for d in range(SIDE)] for a in CHIPS}
    return me, near


def enter(near):
    barrier = pltpu.get_barrier_semaphore()
    for axis in CHIPS:
        for d in (1, 3):
            pl.semaphore_signal(barrier, inc=1, device_id={axis: near[axis][d]}, device_id_type=pl.DeviceIdType.MESH)
    pl.semaphore_wait(barrier, 6)


class Sender:
    def __init__(self, near, send_sem, recv_sem):
        self.near, self.send_sem, self.recv_sem, self.open = near, send_sem, recv_sem, {}

    def put(self, key, src, dst, axis, step):
        copy = pltpu.make_async_remote_copy(
            src_ref=src, dst_ref=dst, send_sem=self.send_sem.at[key], recv_sem=self.recv_sem.at[key],
            device_id={axis: self.near[axis][step]}, device_id_type=pl.DeviceIdType.MESH)
        copy.start()
        self.open[key] = copy

    def got(self, key):
        self.open[key].wait_recv()

    def close(self):
        for copy in self.open.values():
            copy.wait_send()


def gather_kernel(width, src, out, buf, send_sem, recv_sem, loc_sem, out_sem):
    me, near = ring_places()
    mine = {a: me[a] for a in CHIPS}
    jobs = jobs_of(width)
    first = pltpu.make_async_copy(src, view(buf, (slice(None),), CHIPS, mine), loc_sem.at[0])
    first.start()
    enter(near)
    first.wait()
    net = Sender(near, send_sem, recv_sem)
    for phase in range(3):
        def at(job, place, part=None):
            mat, cols, order = jobs[job]
            axis = order[2 - phase]
            sel = {a: me[a] for a in order[:2 - phase]}
            sel[axis] = place
            if part is not None:
                sel.update(half(order[3 - phase], part))
            return view(buf, (mat,), CHIPS, sel, cols)

        def push(job, slot, place, part, step):
            here = at(job, place, part)
            net.put((job, phase, slot), here, here, jobs[job][2][2 - phase], step)

        parts = (None,) if phase == 0 else (0, 1)
        for job in range(len(jobs)):
            places = near[jobs[job][2][2 - phase]]
            if phase == 0:
                push(job, 0, places[0], None, 1)
                push(job, 1, places[0], None, 3)
            else:
                push(job, 0, places[0], 0, 1)
                push(job, 1, places[0], 1, 3)
                push(job, 2, places[0], 1, 1)
                push(job, 3, places[0], 0, 3)
        for job in range(len(jobs)):
            places = near[jobs[job][2][2 - phase]]
            if phase == 0:
                net.got((job, 0, 0))
                push(job, 2, places[3], None, 1)
            else:
                net.got((job, phase, 0))
                push(job, 4, places[3], 0, 1)
                net.got((job, phase, 1))
                push(job, 5, places[1], 1, 3)
        for job in range(len(jobs)):
            for slot in ((1, 2) if phase == 0 else (2, 3, 4, 5)):
                net.got((job, phase, slot))
    last = [pltpu.make_async_copy(buf.at[mat], out.at[mat], out_sem.at[mat]) for mat in range(4)]
    for copy in last:
        copy.start()
    for copy in last:
        copy.wait()
    net.close()


def gather(packed, call_id):
    width = packed.shape[-1]
    full = (4, SIDE, SIDE, SIDE, ROWS, width)
    out = pl.pallas_call(
        functools.partial(gather_kernel, width),
        out_shape=jax.ShapeDtypeStruct(full, packed.dtype),
        in_specs=[pl.BlockSpec(memory_space=pl.ANY)],
        out_specs=pl.BlockSpec(memory_space=pl.ANY),
        scratch_shapes=[pltpu.VMEM(full, packed.dtype), pltpu.SemaphoreType.DMA((6, 3, 6)), pltpu.SemaphoreType.DMA((6, 3, 6)),
                        pltpu.SemaphoreType.DMA((1,)), pltpu.SemaphoreType.DMA((4,))],
        compiler_params=pltpu.CompilerParams(collective_id=call_id, has_side_effects=True),
        name="gather",
    )(packed)
    return out.reshape(4, SIDE ** 3 * ROWS, width)


def add_into(dst, src, lead):
    if not lead:
        dst[...] = dst[...] + src[...]
        return

    def step(k, _):
        add_into(dst.at[k], src.at[k], lead[1:])
        return 0

    lax.fori_loop(0, lead[0], step, 0)


def sum_kernel(width, up, down, out, buf, *rest):
    recv = rest[:18]
    send_sem, recv_sem, loc_sem = rest[18:]
    me, near = ring_places()
    jobs = jobs_of(width)
    net = Sender(near, send_sem, recv_sem)

    def take(mat):
        return (up if mat < 2 else down), mat % 2

    loads = {}
    for d in (2, 1, 3, 0):
        for job, (mat, cols, order) in enumerate(jobs):
            sel = {order[0]: near[order[0]][d]}
            ref, k = take(mat)
            loads[job, d] = pltpu.make_async_copy(view(ref, (k,), CHIPS, sel, cols), view(buf, (mat,), CHIPS, sel, cols),
                                                  loc_sem.at[job, d])
            loads[job, d].start()
    enter(near)
    for phase in range(3):
        def here(job, d, part=None):
            mat, cols, order = jobs[job]
            sel = {a: me[a] for a in order[:phase]}
            sel[order[phase]] = near[order[phase]][d]
            if part is not None:
                sel.update(half(order[phase + 1], part))
            return view(buf, (mat,), CHIPS, sel, cols)

        def there(job, slot, part=None):
            order = jobs[job][2]
            left = [a for a in CHIPS if a not in order[:phase + 1]]
            sel = {} if part is None else half(order[phase + 1], part)
            return view(recv[3 * job + phase], (slot,), left, sel)

        def lead(job, part=None):
            order = jobs[job][2]
            return [2 if part is not None and a == order[phase + 1] else SIDE for a in CHIPS if a not in order[:phase + 1]]

        def push(job, slot, d, part, to_slot, step):
            net.put((job, phase, slot), here(job, d, part), there(job, to_slot, part), jobs[job][2][phase], step)

        for job in range(len(jobs)):
            if phase == 0:
                loads[job, 2].wait()
            if phase == 2:
                push(job, 0, 2, None, 0, 1)
                push(job, 3, 3, None, 2, 3)
            else:
                push(job, 0, 2, 0, 0, 1)
                push(job, 1, 2, 1, 0, 3)
        for job in range(len(jobs)):
            if phase == 0:
                loads[job, 1].wait()
                loads[job, 3].wait()
            if phase < 2:
                push(job, 2, 1, 1, 1, 1)
                push(job, 3, 3, 0, 2, 3)
        for job in range(len(jobs)):
            net.got((job, phase, 0))
            if phase == 2:
                add_into(here(job, 1), there(job, 0), [])
                push(job, 2, 1, None, 1, 1)
            else:
                add_into(here(job, 1, 0), there(job, 0, 0), lead(job, 0))
                push(job, 4, 1, 0, 1, 1)
                net.got((job, phase, 1))
                add_into(here(job, 3, 1), there(job, 0, 1), lead(job, 1))
                push(job, 5, 3, 1, 2, 3)
        for job in range(len(jobs)):
            if phase == 0:
                loads[job, 0].wait()
            for slot in ((2, 3) if phase == 2 else (2, 3, 4, 5)):
                net.got((job, phase, slot))
            add_into(here(job, 0), there(job, 1), lead(job))
            add_into(here(job, 0), there(job, 2), lead(job))
    for mat in range(4):
        out[mat] = view(buf, (mat,), CHIPS, me)[...]
    net.close()


def scatter_sum(up, down, call_id):
    width = up.shape[-1]
    full = (SIDE, SIDE, SIDE, ROWS, width)
    blocks = []
    for mat, cols, order in jobs_of(width):
        blocks += [pltpu.VMEM((3,) + (SIDE,) * (2 - phase) + (ROWS, cols[1]), F32) for phase in range(3)]
    return pl.pallas_call(
        functools.partial(sum_kernel, width),
        out_shape=jax.ShapeDtypeStruct((4, ROWS, width), F32),
        in_specs=[pl.BlockSpec(memory_space=pl.ANY)] * 2,
        out_specs=pl.BlockSpec(memory_space=pltpu.VMEM),
        scratch_shapes=[pltpu.VMEM((4,) + full, F32)] + blocks
        + [pltpu.SemaphoreType.DMA((6, 3, 6)), pltpu.SemaphoreType.DMA((6, 3, 6)), pltpu.SemaphoreType.DMA((6, 4))],
        compiler_params=pltpu.CompilerParams(collective_id=call_id, has_side_effects=True),
        name="scatter_sum",
    )(up.reshape((2,) + full), down.reshape((2,) + full))


def pack_weights(up_loc, down_loc, core):
    layers, up_rows, hidden = up_loc.shape
    by_core = up_loc.reshape(layers, up_rows, 64, 2, 2, 16)
    mine = lax.dynamic_index_in_dim(by_core, core, 3, keepdims=False)
    other = lax.dynamic_index_in_dim(by_core, 1 - core, 3, keepdims=False)
    mine, other = (v.transpose(0, 3, 1, 2, 4).reshape(layers, 2, up_rows, hidden // 4) for v in (mine, other))
    got = swap(other)
    up = jnp.where(core == 0, jnp.concatenate([mine, got], 2), jnp.concatenate([got, mine], 2))
    return jnp.concatenate([up, down_loc.reshape(layers, 2, 16, -1)], 1)


def unpack_up_grad(grad, core):
    layers = grad.shape[0]
    rows = grad.reshape(layers, 2, 2, 8, 64, 16)
    mine = lax.dynamic_index_in_dim(rows, core, 2, keepdims=False)
    got = swap(lax.dynamic_index_in_dim(rows, 1 - core, 2, keepdims=False))
    both = jnp.where(core == 0, jnp.stack([mine, got]), jnp.stack([got, mine]))
    return both.transpose(1, 3, 4, 0, 2, 5).reshape(layers, 8, 4096)


def solution(mesh):
    grid = Mesh(mesh.devices.reshape(SIDE, SIDE, SIDE, 2), ALL)
    tok_spec = P(ALL, None)
    weight_spec = P(None, ALL, None)

    def device_step(x_loc, up_loc, down_loc, g_loc):
        layers = up_loc.shape[0]
        tokens = x_loc.shape[0]
        core = lax.axis_index("c")
        packed = pack_weights(up_loc, down_loc, core)
        x_cur = pair_rows(x_loc, core)
        g_cur = pair_rows(g_loc, core)
        saved = []
        for layer in range(layers):
            full = gather(packed[layer], layer)
            pre = [dot("tk,kn->tn", x_cur, full[j]) for j in range(2)]
            act = [gelu_parts(p)[0].astype(BF16) for p in pre]
            part = dot("tn,nm->tm", act[0], full[2]) + dot("tn,nm->tm", act[1], full[3])
            saved.append((x_cur, pre, act))
            x_cur = (x_cur.astype(F32) + (part + swap(part))).astype(BF16)
        y_out = lax.dynamic_slice_in_dim(x_cur, core * tokens, tokens, 0)
        mark = x_cur
        grads = [None] * layers
        for layer in reversed(range(layers)):
            again, _ = lax.optimization_barrier((packed[layer], mark))
            full = gather(again, layers + layer)
            x_in, pre, act = saved[layer]
            d_pre = [(dot("tm,nm->tn", g_cur, full[2 + j]) * gelu_parts(pre[j])[1]).astype(BF16) for j in range(2)]
            grad_down = jnp.stack([dot("tn,tm->nm", act[j], g_cur) for j in range(2)])
            grad_up = jnp.stack([dot("tk,tn->kn", x_in, d_pre[j]) for j in range(2)])
            part = dot("tn,kn->tk", d_pre[0], full[0]) + dot("tn,kn->tk", d_pre[1], full[1])
            g_cur = (g_cur.astype(F32) + (part + swap(part))).astype(BF16)
            grads[layer] = scatter_sum(grad_up, grad_down, 2 * layers + layer)
            mark = g_cur
        grads = jnp.stack(grads)
        grad_up = unpack_up_grad(grads[:, :2], core)
        grad_in = lax.dynamic_slice_in_dim(g_cur, core * tokens, tokens, 0)
        return y_out, grad_in, grad_up, grads[:, 2:].reshape(layers, 32, -1)

    return jax.shard_map(device_step, mesh=grid, in_specs=(tok_spec, weight_spec, weight_spec, tok_spec),
                         out_specs=(tok_spec, tok_spec, weight_spec, weight_spec), check_vma=False)
```

```python
import functools
import math

import jax
import jax.numpy as jnp
from jax import lax
from jax.experimental import pallas as pl
from jax.experimental.pallas import tpu as pltpu
from jax.sharding import Mesh, PartitionSpec as P

CHIPS = ("z", "y", "x")
ALL = CHIPS + ("c",)
BF16 = jnp.bfloat16
F32 = jnp.float32
SIDE = 4
ROWS = 16
TILE = 256
WIDE = 512
INV_SQRT_2PI = (2.0 * math.pi) ** -0.5
VMEM_LIMIT = 63 * 1024 * 1024
MESH = pl.DeviceIdType.MESH
ORDERS = (("x", "y", "z"), ("y", "z", "x"), ("z", "x", "y"))


def gelu_parts(pre_act):
    norm_cdf = 0.5 * (1.0 + lax.erf(pre_act * (2.0 ** -0.5)))
    norm_pdf = jnp.exp(-0.5 * pre_act * pre_act) * INV_SQRT_2PI
    return pre_act * norm_cdf, norm_cdf + pre_act * norm_pdf


def swap(val):
    return lax.ppermute(val, "c", [(0, 1), (1, 0)])


def pair_rows(own, core):
    got = swap(own)
    return jnp.where(core == 0, jnp.concatenate([own, got], 0), jnp.concatenate([got, own], 0))


def jobs_of(width):
    tile = width // 8
    cuts = ((0, 3 * tile), (3 * tile, 3 * tile), (6 * tile, 2 * tile))
    return [(3, cuts[k], ORDERS[k]) for k in range(3)] + [(mat, (0, width), ORDERS[mat]) for mat in range(3)]


SMALL, LARGE = range(3), range(3, 6)


def view(ref, lead, axes, sel, cols=None):
    mid = tuple(sel.get(a, slice(None)) for a in axes)
    last = (slice(None), pl.ds(*cols)) if cols is not None else ()
    return ref.at[lead + mid + last]


def half(axis, k):
    return {axis: pl.ds(2 * k, 2)}


def ring_places():
    me = {a: lax.axis_index(a) for a in CHIPS}
    near = {a: [lax.rem(me[a] + d, SIDE) for d in range(SIDE)] for a in CHIPS}
    return me, near


def enter(near, ring=True, partner=None):
    barrier = pltpu.get_barrier_semaphore()
    if ring:
        for axis in CHIPS:
            for d in (1, 3):
                pl.semaphore_signal(barrier, inc=1, device_id={axis: near[axis][d]}, device_id_type=MESH)
    if partner is not None:
        pl.semaphore_signal(barrier, inc=1, device_id={"c": partner}, device_id_type=MESH)
    pl.semaphore_wait(barrier, 6 * ring + (partner is not None))


class Sender:
    def __init__(self, near, send_sem, recv_sem):
        self.near, self.send_sem, self.recv_sem, self.open = near, send_sem, recv_sem, {}

    def put(self, key, src, dst, axis, step):
        copy = pltpu.make_async_remote_copy(
            src_ref=src, dst_ref=dst, send_sem=self.send_sem.at[key], recv_sem=self.recv_sem.at[key],
            device_id={axis: self.near[axis][step]}, device_id_type=MESH)
        copy.start()
        self.open[key] = copy

    def got(self, key):
        self.open[key].wait_recv()

    def close(self):
        for copy in self.open.values():
            copy.wait_send()


RING_SEMS = [pltpu.SemaphoreType.DMA((6, 3, 6)), pltpu.SemaphoreType.DMA((6, 3, 6))]


class Gather:
    def __init__(self, width, me, near, buf, send_sem, recv_sem):
        self.me, self.near, self.buf, self.jobs = me, near, buf, jobs_of(width)
        self.net = Sender(near, send_sem, recv_sem)

    def push(self, job, phase, slot, d, part, step):
        mat, cols, order = self.jobs[job]
        axis = order[2 - phase]
        sel = {a: self.me[a] for a in order[:2 - phase]}
        sel[axis] = self.near[axis][d]
        if part is not None:
            sel.update(half(order[3 - phase], part))
        here = view(self.buf, (mat,), CHIPS, sel, cols)
        self.net.put((job, phase, slot), here, here, axis, step)

    def send(self, phase):
        for job in range(6):
            if phase == 0:
                self.push(job, phase, 0, 0, None, 1)
                self.push(job, phase, 1, 0, None, 3)
            else:
                self.push(job, phase, 0, 0, 0, 1)
                self.push(job, phase, 1, 0, 1, 3)
                self.push(job, phase, 2, 0, 1, 1)
                self.push(job, phase, 3, 0, 0, 3)

    def forward(self, phase):
        for job in range(6):
            self.net.got((job, phase, 0))
            if phase == 0:
                self.push(job, phase, 2, 3, None, 1)
            else:
                self.push(job, phase, 4, 3, 0, 1)
                self.net.got((job, phase, 1))
                self.push(job, phase, 5, 1, 1, 3)

    def finish(self, phase):
        for job in range(6):
            for slot in ((1, 2) if phase == 0 else (2, 3, 4, 5)):
                self.net.got((job, phase, slot))

    def begin(self):
        for phase in range(2):
            self.send(phase)
            self.forward(phase)
            self.finish(phase)
        self.send(2)


def gather_kernel(width, src, out, buf, send_sem, recv_sem, loc_sem, out_sem):
    me, near = ring_places()
    first = pltpu.make_async_copy(src, view(buf, (slice(None),), CHIPS, me), loc_sem.at[0])
    first.start()
    enter(near)
    first.wait()
    ring = Gather(width, me, near, buf, send_sem, recv_sem)
    ring.begin()
    ring.forward(2)
    ring.finish(2)
    last = pltpu.make_async_copy(buf, out, out_sem.at[0])
    last.start()
    last.wait()
    ring.net.close()


def gather(packed, call_id):
    width = packed.shape[-1]
    full = (4, SIDE, SIDE, SIDE, ROWS, width)
    return pl.pallas_call(
        functools.partial(gather_kernel, width),
        out_shape=jax.ShapeDtypeStruct(full, packed.dtype),
        in_specs=[pl.BlockSpec(memory_space=pl.ANY)],
        out_specs=pl.BlockSpec(memory_space=pl.ANY),
        scratch_shapes=[pltpu.VMEM(full, packed.dtype)] + RING_SEMS
        + [pltpu.SemaphoreType.DMA((1,)), pltpu.SemaphoreType.DMA((1,))],
        compiler_params=pltpu.CompilerParams(collective_id=call_id, has_side_effects=True),
        name="gather",
    )(packed)


def dot_nn(left, right):
    return lax.dot_general(left, right, (((1,), (0,)), ((), ())), preferred_element_type=F32)


def dot_nt(left, right):
    return lax.dot_general(left, right, (((1,), (1,)), ((), ())), preferred_element_type=F32)


def dot_tn(left, right):
    return lax.dot_general(left, right, (((0,), (0,)), ((), ())), preferred_element_type=F32)


def layer_kernel(forward, width, with_gather, *refs):
    refs = list(refs)
    stream, weights = refs.pop(0), refs.pop(0)
    slope_in = None if forward else refs.pop(0)
    packed = refs.pop(0) if with_gather else None
    result = refs.pop(0)
    act_out = refs.pop(0)
    slope_out = refs.pop(0) if forward else None
    next_out = refs.pop(0) if with_gather else None
    cur, mats, act, slope, part, got, pair_send, pair_recv, loc_sem, out_sem = refs[:10]
    tokens = cur.shape[0]
    tiles = tokens // TILE
    me, near = ring_places()
    partner = 1 - lax.axis_index("c")
    loads = [pltpu.make_async_copy(stream, cur, loc_sem.at[0]), pltpu.make_async_copy(weights, mats, loc_sem.at[1])]
    if not forward:
        loads.append(pltpu.make_async_copy(slope_in, slope, loc_sem.at[2]))
    if with_gather:
        buf, send_sem, recv_sem = refs[10:]
        ring = Gather(width, me, near, buf, send_sem, recv_sem)
        own = pltpu.make_async_copy(packed, view(buf, (slice(None),), CHIPS, me), loc_sem.at[3])
        own.start()
    for copy in loads:
        copy.start()
    enter(near, with_gather, partner)
    if with_gather:
        own.wait()
        ring.begin()
    for copy in loads:
        copy.wait()

    def exchange(tile):
        rows = pl.ds(tile * TILE, TILE)
        return pltpu.make_async_remote_copy(
            src_ref=part.at[rows], dst_ref=got.at[rows], send_sem=pair_send.at[tile], recv_sem=pair_recv.at[tile],
            device_id={"c": partner}, device_id_type=MESH)

    def compute(tile, _):
        rows = pl.ds(pl.multiple_of(tile * TILE, TILE), TILE)
        left = cur[rows, :]
        for block in range(2):
            for cut in range(width // WIDE):
                cols = pl.ds(block * width + cut * WIDE, WIDE)
                if forward:
                    pre = dot_nn(left, mats[block * width:(block + 1) * width, cut * WIDE:(cut + 1) * WIDE])
                    act_val, slope_val = gelu_parts(pre)
                    act[rows, cols] = act_val.astype(BF16)
                    slope[rows, cols] = slope_val
                else:
                    low = (2 + block) * width + cut * WIDE
                    d_act = dot_nt(left, mats[low:low + WIDE, :])
                    act[rows, cols] = (d_act * slope[rows, cols]).astype(BF16)
        if forward:
            part[rows, :] = dot_nn(act[rows, :], mats[2 * width:, :])
        else:
            part[rows, :] = dot_nt(act[rows, :width], mats[:width, :]) + dot_nt(act[rows, width:], mats[width:2 * width, :])
        exchange(tile).start()
        return 0

    saves = []

    def save(k, low, high):
        rows = pl.ds(low * TILE, (high - low) * TILE)
        pairs = [(act, act_out)] + ([(slope, slope_out)] if forward else [])
        for n, (src, dst) in enumerate(pairs):
            saves.append(pltpu.make_async_copy(src.at[rows], dst.at[rows], out_sem.at[2 * k + n]))
            saves[-1].start()

    mid = tiles // 2
    lax.fori_loop(0, mid, compute, 0)
    save(0, 0, mid)
    if with_gather:
        ring.forward(2)
    lax.fori_loop(mid, tiles, compute, 0)
    save(1, mid, tiles)
    for tile in range(tiles):
        exchange(tile).wait_recv()
        rows = pl.ds(tile * TILE, TILE)
        result[rows, :] = (cur[rows, :].astype(F32) + (part[rows, :] + got[rows, :])).astype(BF16)
    if with_gather:
        ring.finish(2)
        last = pltpu.make_async_copy(buf, next_out, out_sem.at[4])
        last.start()
        last.wait()
        ring.net.close()
    for copy in saves:
        copy.wait()
    for tile in range(tiles):
        exchange(tile).wait_send()


def layer_call(forward, stream, full, slope, packed, call_id):
    tokens, width = stream.shape
    hidden = 2 * width
    with_gather = packed is not None
    shape = jax.ShapeDtypeStruct
    whole = (4, SIDE, SIDE, SIDE, ROWS, width)
    args = [stream, full.reshape(4 * width, width)] + ([] if forward else [slope]) + ([packed] if with_gather else [])
    outs = [shape((tokens, width), BF16), shape((tokens, hidden), BF16)]
    outs += ([shape((tokens, hidden), F32)] if forward else []) + ([shape(whole, BF16)] if with_gather else [])
    tiles = tokens // TILE
    return pl.pallas_call(
        functools.partial(layer_kernel, forward, width, with_gather),
        out_shape=outs,
        in_specs=[pl.BlockSpec(memory_space=pl.ANY)] * len(args),
        out_specs=[pl.BlockSpec(memory_space=pltpu.VMEM)] + [pl.BlockSpec(memory_space=pl.ANY)] * (len(outs) - 1),
        scratch_shapes=[pltpu.VMEM((tokens, width), BF16), pltpu.VMEM((4 * width, width), BF16),
                        pltpu.VMEM((tokens, hidden), BF16), pltpu.VMEM((tokens, hidden), F32),
                        pltpu.VMEM((tokens, width), F32), pltpu.VMEM((tokens, width), F32),
                        pltpu.SemaphoreType.DMA((tiles,)), pltpu.SemaphoreType.DMA((tiles,)),
                        pltpu.SemaphoreType.DMA((4,)), pltpu.SemaphoreType.DMA((5,))]
        + ([pltpu.VMEM(whole, BF16)] + RING_SEMS if with_gather else []),
        compiler_params=pltpu.CompilerParams(collective_id=call_id, has_side_effects=True, vmem_limit_bytes=VMEM_LIMIT),
        cost_estimate=pl.CostEstimate(flops=8 * tokens * hidden * width, bytes_accessed=40 << 20, transcendentals=0),
        name="forward_layer" if forward else "backward_layer",
    )(*args)


def add_into(dst, src, lead):
    if not lead:
        dst[...] = dst[...] + src[...]
        return

    def step(k, _):
        add_into(dst.at[k], src.at[k], lead[1:])
        return 0

    lax.fori_loop(0, lead[0], step, 0)


class RingSum:
    def __init__(self, width, me, near, buf, recv, send_sem, recv_sem):
        self.me, self.near, self.buf, self.recv, self.jobs = me, near, buf, recv, jobs_of(width)
        self.net = Sender(near, send_sem, recv_sem)

    def here(self, job, phase, d, part=None):
        mat, cols, order = self.jobs[job]
        sel = {a: self.me[a] for a in order[:phase]}
        sel[order[phase]] = self.near[order[phase]][d]
        if part is not None:
            sel.update(half(order[phase + 1], part))
        return view(self.buf, (mat,), CHIPS, sel, cols)

    def there(self, job, phase, slot, part=None):
        order = self.jobs[job][2]
        left = [a for a in CHIPS if a not in order[:phase + 1]]
        return view(self.recv[3 * job + phase], (slot,), left, {} if part is None else half(order[phase + 1], part))

    def lead(self, job, phase, part=None):
        order = self.jobs[job][2]
        return [2 if part is not None and a == order[phase + 1] else SIDE for a in CHIPS if a not in order[:phase + 1]]

    def push(self, job, phase, slot, d, part, to_slot, step):
        self.net.put((job, phase, slot), self.here(job, phase, d, part), self.there(job, phase, to_slot, part),
                     self.jobs[job][2][phase], step)

    def send(self, job, phase):
        if phase == 2:
            self.push(job, phase, 0, 2, None, 0, 1)
            self.push(job, phase, 3, 3, None, 2, 3)
        else:
            self.push(job, phase, 0, 2, 0, 0, 1)
            self.push(job, phase, 1, 2, 1, 0, 3)
            self.push(job, phase, 2, 1, 1, 1, 1)
            self.push(job, phase, 3, 3, 0, 2, 3)

    def mid(self, job, phase):
        self.net.got((job, phase, 0))
        if phase == 2:
            add_into(self.here(job, phase, 1), self.there(job, phase, 0), [])
            self.push(job, phase, 2, 1, None, 1, 1)
        else:
            add_into(self.here(job, phase, 1, 0), self.there(job, phase, 0, 0), self.lead(job, phase, 0))
            self.push(job, phase, 4, 1, 0, 1, 1)
            self.net.got((job, phase, 1))
            add_into(self.here(job, phase, 3, 1), self.there(job, phase, 0, 1), self.lead(job, phase, 1))
            self.push(job, phase, 5, 3, 1, 2, 3)

    def finish(self, job, phase):
        for slot in ((2, 3) if phase == 2 else (2, 3, 4, 5)):
            self.net.got((job, phase, slot))
        add_into(self.here(job, phase, 0), self.there(job, phase, 1), self.lead(job, phase))
        add_into(self.here(job, phase, 0), self.there(job, phase, 2), self.lead(job, phase))


def recv_blocks(width):
    blocks = []
    for mat, cols, order in jobs_of(width):
        blocks += [pltpu.VMEM((3,) + (SIDE,) * (2 - phase) + (ROWS, cols[1]), F32) for phase in range(3)]
    return blocks


def sum_kernel(width, x_ref, act_ref, d_pre_ref, g_ref, out, x_val, act_val, d_pre, g_val, buf, *rest):
    send_sem, recv_sem, loc_sem = rest[18:]
    me, near = ring_places()
    ring = RingSum(width, me, near, buf, rest[:18], send_sem, recv_sem)
    loads = [pltpu.make_async_copy(src, dst, loc_sem.at[k]) for k, (src, dst) in enumerate(
        ((act_ref, act_val), (g_ref, g_val), (x_ref, x_val), (d_pre_ref, d_pre)))]
    for copy in loads:
        copy.start()
    enter(near)

    def grad(mat):
        def slab(z, _):
            if mat < 2:
                cols = pl.ds(pl.multiple_of(z * (width // SIDE), width // SIDE), width // SIDE)
                val = dot_tn(x_val[:, cols], d_pre[:, mat * width:(mat + 1) * width])
            else:
                cols = pl.ds(pl.multiple_of((mat - 2) * width + z * (width // SIDE), width // SIDE), width // SIDE)
                val = dot_tn(act_val[:, cols], g_val[...])
            buf[mat, z] = val.reshape(SIDE, SIDE, ROWS, width)
            return 0

        lax.fori_loop(0, SIDE, slab, 0)

    loads[0].wait()
    loads[1].wait()
    grad(3)
    for job in SMALL:
        ring.send(job, 0)
    grad(2)
    ring.send(5, 0)
    loads[2].wait()
    loads[3].wait()
    for mat in range(2):
        grad(mat)
        ring.send(3 + mat, 0)
    for job in SMALL:
        ring.mid(job, 0)
    for job in LARGE:
        ring.mid(job, 0)
    for phase in range(3):
        for group in (SMALL, LARGE):
            for job in group:
                ring.finish(job, phase)
                if phase < 2:
                    ring.send(job, phase + 1)
        if phase < 2:
            for group in (SMALL, LARGE):
                for job in group:
                    ring.mid(job, phase + 1)
    for mat in range(4):
        out[mat] = view(buf, (mat,), CHIPS, me)[...]
    ring.net.close()


def scatter_sum(x_in, act, d_pre, g_in, call_id):
    tokens, width = x_in.shape
    return pl.pallas_call(
        functools.partial(sum_kernel, width),
        out_shape=jax.ShapeDtypeStruct((4, ROWS, width), F32),
        in_specs=[pl.BlockSpec(memory_space=pl.ANY)] * 4,
        out_specs=pl.BlockSpec(memory_space=pltpu.VMEM),
        scratch_shapes=[pltpu.VMEM((tokens, width), BF16), pltpu.VMEM((tokens, 2 * width), BF16),
                        pltpu.VMEM((tokens, 2 * width), BF16), pltpu.VMEM((tokens, width), BF16),
                        pltpu.VMEM((4, SIDE, SIDE, SIDE, ROWS, width), F32)] + recv_blocks(width)
        + RING_SEMS + [pltpu.SemaphoreType.DMA((4,))],
        compiler_params=pltpu.CompilerParams(collective_id=call_id, has_side_effects=True, vmem_limit_bytes=VMEM_LIMIT),
        cost_estimate=pl.CostEstimate(flops=8 * tokens * width * width, bytes_accessed=12 << 20, transcendentals=0),
        name="scatter_sum",
    )(x_in, act, d_pre, g_in)


def pack_weights(up_loc, down_loc, core):
    layers, up_rows, hidden = up_loc.shape
    by_core = up_loc.reshape(layers, up_rows, 64, 2, 2, 16)
    mine = lax.dynamic_index_in_dim(by_core, core, 3, keepdims=False)
    other = lax.dynamic_index_in_dim(by_core, 1 - core, 3, keepdims=False)
    mine, other = (v.transpose(0, 3, 1, 2, 4).reshape(layers, 2, up_rows, hidden // 4) for v in (mine, other))
    got = swap(other)
    up = jnp.where(core == 0, jnp.concatenate([mine, got], 2), jnp.concatenate([got, mine], 2))
    return jnp.concatenate([up, down_loc.reshape(layers, 2, 16, -1)], 1)


def unpack_up_grad(grad, core):
    layers = grad.shape[0]
    rows = grad.reshape(layers, 2, 2, 8, 64, 16)
    mine = lax.dynamic_index_in_dim(rows, core, 2, keepdims=False)
    got = swap(lax.dynamic_index_in_dim(rows, 1 - core, 2, keepdims=False))
    both = jnp.where(core == 0, jnp.stack([mine, got]), jnp.stack([got, mine]))
    return both.transpose(1, 3, 4, 0, 2, 5).reshape(layers, 8, 4096)


def solution(mesh):
    grid = Mesh(mesh.devices.reshape(SIDE, SIDE, SIDE, 2), ALL)
    tok_spec = P(ALL, None)
    weight_spec = P(None, ALL, None)

    def device_step(x_loc, up_loc, down_loc, g_loc):
        layers = up_loc.shape[0]
        tokens = x_loc.shape[0]
        core = lax.axis_index("c")
        packed = pack_weights(up_loc, down_loc, core)
        x_cur = pair_rows(x_loc, core)
        g_cur = pair_rows(g_loc, core)
        saved = []
        full = gather(packed[0], 0)
        for layer in range(layers):
            following = packed[layer + 1] if layer + 1 < layers else lax.optimization_barrier((packed[layer], x_cur))[0]
            x_in = x_cur
            x_cur, act, slope, full = layer_call(True, x_in, full, None, following, 1 + layer)
            saved.append((x_in, act, slope))
        y_out = lax.dynamic_slice_in_dim(x_cur, core * tokens, tokens, 0)
        grads = [None] * layers
        for layer in reversed(range(layers)):
            x_in, act, slope = saved[layer]
            g_in = g_cur
            if layer:
                following = lax.optimization_barrier((packed[layer - 1], x_cur))[0]
                g_cur, d_pre, full = layer_call(False, g_in, full, slope, following, 4 + layer)
            else:
                g_cur, d_pre = layer_call(False, g_in, full, slope, None, 4 + layer)
            grads[layer] = scatter_sum(x_in, act, d_pre, g_in, 7 + layer)
        grads = jnp.stack(grads)
        grad_up = unpack_up_grad(grads[:, :2], core)
        grad_in = lax.dynamic_slice_in_dim(g_cur, core * tokens, tokens, 0)
        return y_out, grad_in, grad_up, grads[:, 2:].reshape(layers, 32, -1)

    return jax.shard_map(device_step, mesh=grid, in_specs=(tok_spec, weight_spec, weight_spec, tok_spec),
                         out_specs=(tok_spec, tok_spec, weight_spec, weight_spec), check_vma=False)
```

```python
import functools
import math

import jax
import jax.numpy as jnp
from jax import lax
from jax.experimental import pallas as pl
from jax.experimental.pallas import tpu as pltpu
from jax.sharding import Mesh, PartitionSpec as P

CHIPS = ("z", "y", "x")
ALL = CHIPS + ("c",)
BF16 = jnp.bfloat16
F32 = jnp.float32
SIDE = 4
ROWS = 16
TILE = 256
WIDE = 512
INV_SQRT_2PI = (2.0 * math.pi) ** -0.5
VMEM_LIMIT = 63 * 1024 * 1024
MESH = pl.DeviceIdType.MESH
HERE, NEXT, OPPOSITE, PREV = range(4)
FULL = None
ORDERS = (("x", "y", "z"), ("y", "z", "x"), ("z", "x", "y"))


def gelu_parts(pre_act):
    norm_cdf = 0.5 * (1.0 + lax.erf(pre_act * (2.0 ** -0.5)))
    norm_pdf = jnp.exp(-0.5 * pre_act * pre_act) * INV_SQRT_2PI
    return pre_act * norm_cdf, norm_cdf + pre_act * norm_pdf


def jobs_of(width):
    tile = width // 8
    cuts = ((0, 3 * tile), (3 * tile, 3 * tile), (6 * tile, 2 * tile))
    return [(3, cuts[k], ORDERS[k]) for k in range(3)] + [(mat, (0, width), ORDERS[mat]) for mat in range(3)]


JOBS = range(6)
SMALL, LARGE = JOBS[:3], JOBS[3:]


def view(ref, lead, axes, sel, cols=None):
    mid = tuple(sel.get(a, slice(None)) for a in axes)
    last = (slice(None), pl.ds(*cols)) if cols is not None else ()
    return ref.at[lead + mid + last]


def half(axis, k):
    return {axis: pl.ds(2 * k, 2)}


def ring_places():
    me = {a: lax.axis_index(a) for a in CHIPS}
    near = {a: [lax.rem(me[a] + d, SIDE) for d in range(SIDE)] for a in CHIPS}
    return me, near


def enter(near, ring=True, partner=None):
    barrier = pltpu.get_barrier_semaphore()
    if ring:
        for axis in CHIPS:
            for d in (1, 3):
                pl.semaphore_signal(barrier, inc=1, device_id={axis: near[axis][d]}, device_id_type=MESH)
    if partner is not None:
        pl.semaphore_signal(barrier, inc=1, device_id={"c": partner}, device_id_type=MESH)
    pl.semaphore_wait(barrier, 6 * ring + (partner is not None))


class Sender:
    def __init__(self, near, send_sem, recv_sem):
        self.near, self.send_sem, self.recv_sem, self.open = near, send_sem, recv_sem, {}

    def put(self, key, src, dst, axis, step):
        copy = pltpu.make_async_remote_copy(
            src_ref=src, dst_ref=dst, send_sem=self.send_sem.at[key], recv_sem=self.recv_sem.at[key],
            device_id={axis: self.near[axis][step]}, device_id_type=MESH)
        copy.start()
        self.open[key] = copy

    def got(self, key):
        self.open[key].wait_recv()

    def close(self):
        for copy in self.open.values():
            copy.wait_send()


RING_SEMS = [pltpu.SemaphoreType.DMA((6, 3, 6)), pltpu.SemaphoreType.DMA((6, 3, 6))]


class Gather:
    def __init__(self, width, me, near, net, buf, lead=(), skip=0):
        self.me, self.near, self.net, self.buf, self.jobs = me, near, net, buf, jobs_of(width)
        self.lead, self.skip = lead, skip

    def block(self, job, fixed, more=None, ref=None, skip=None):
        mat, cols, order = self.jobs[job]
        skip = self.skip if skip is None else skip
        sel = {a: self.me[a] for a in order[:fixed]}
        sel.update(more or {})
        lead = self.lead if ref is None else ()
        return view(self.buf if ref is None else ref, lead + (mat,), [a for a in CHIPS if a not in order[:skip]], sel, cols)

    def push(self, job, phase, slot, d, part, step):
        order = self.jobs[job][2]
        axis = order[2 - phase]
        sel = {axis: self.near[axis][d]}
        if part is not None:
            sel.update(half(order[3 - phase], part))
        here = self.block(job, 2 - phase, sel)
        self.net.put((job, phase, slot), here, here, axis, step)

    def send(self, phase):
        halves = ((FULL, NEXT), (FULL, PREV)) if phase == 0 else ((0, NEXT), (1, PREV), (1, NEXT), (0, PREV))
        for job in JOBS:
            for slot, (part, step) in enumerate(halves):
                self.push(job, phase, slot, HERE, part, step)

    def forward(self, phase):
        for job in JOBS:
            self.net.got((job, phase, 0))
            if phase == 0:
                self.push(job, phase, 2, PREV, FULL, NEXT)
            else:
                self.push(job, phase, 4, PREV, 0, NEXT)
                self.net.got((job, phase, 1))
                self.push(job, phase, 5, NEXT, 1, PREV)

    def finish(self, phase):
        for job in JOBS:
            for slot in ((1, 2) if phase == 0 else (2, 3, 4, 5)):
                self.net.got((job, phase, slot))

    def through(self, phase):
        self.send(phase)
        self.forward(phase)
        self.finish(phase)

    def load(self, src, fixed, sems):
        return [pltpu.make_async_copy(self.block(job, fixed, ref=src, skip=fixed, more=None), self.block(job, fixed), sems.at[job])
                for job in JOBS]

    def store(self, out, d, sems):
        for job in JOBS:
            axis = self.jobs[job][2][0]
            sel = {axis: self.near[axis][d]}
            copy = pltpu.make_async_copy(self.block(job, 0, sel), self.block(job, 0, sel, ref=out), sems.at[job, d])
            copy.start()
            self.stores.append(copy)

    def last_sends(self, out, sems):
        self.stores = []
        self.send(2)
        self.store(out, HERE, sems)

    def close_out(self, out, sems):
        for slots, places in (((2, 3), (NEXT, PREV)), ((4, 5), (OPPOSITE,))):
            for job in JOBS:
                for slot in slots:
                    self.net.got((job, 2, slot))
            for d in places:
                self.store(out, d, sems)
        for copy in self.stores:
            copy.wait()


def column_places(rows, cols):
    src = lax.broadcasted_iota(jnp.int32, (rows, cols), 0)
    dst = lax.broadcasted_iota(jnp.int32, (rows, cols), 1)
    want = ((dst & 127) >> 4) * 64 + (dst >> 8) * 32 + ((dst >> 7) & 1) * 16 + (dst & 15)
    return jnp.where(src == want, 1.0, 0.0).astype(BF16)


def open_kernel(width, up, down, x_ref, g_ref, x_out, g_out, packed_out, full_out, quarter_out, line_out_0, line_out_1,
                perm, pack, x_val, g_val, buf, quarter, lines, send_a, recv_a, send_b, recv_b, send_c, recv_c,
                loc_sem, pair_send, pair_recv, line_sem, quarter_sem, store_sem):
    me, near = ring_places()
    core = lax.axis_index("c")
    tokens = x_ref.shape[0]
    mine = pl.ds(pl.multiple_of(core * tokens, tokens), tokens)
    rows = pl.ds(pl.multiple_of(core * 8, 8), 8)
    local = [pltpu.make_async_copy(down, pack.at[:, 2:4], loc_sem.at[0]),
             pltpu.make_async_copy(x_ref, x_val.at[mine], loc_sem.at[1]),
             pltpu.make_async_copy(g_ref, g_val.at[mine], loc_sem.at[2])]
    for copy in local:
        copy.start()
    enter(near, True, 1 - core)
    places = column_places(512, 512)
    flat = up[...].reshape(24, 4 * width)
    for group in range(4 * width // 512):
        moved = lax.dot_general(flat[:, group * 512:(group + 1) * 512], places, (((1,), (0,)), ((), ())),
                                preferred_element_type=F32).astype(BF16)
        for k in range(4):
            perm[:, k // 2, k % 2, :, group * 128:(group + 1) * 128] = moved[:, k * 128:(k + 1) * 128].reshape(3, 8, 128)
    pair = [pltpu.make_async_remote_copy(src_ref=src, dst_ref=dst, send_sem=pair_send.at[k], recv_sem=pair_recv.at[k],
                                         device_id={"c": 1 - core}, device_id_type=MESH)
            for k, (src, dst) in enumerate(((perm.at[:, 1 - core], pack.at[:, 0:2, rows]),
                                            (x_ref, x_val.at[mine]), (g_ref, g_val.at[mine])))]
    for copy in pair[1:]:
        copy.start()
    pair[0].start()
    own = pltpu.make_async_copy(perm.at[:, core], pack.at[:, 0:2, rows], loc_sem.at[3])
    own.start()
    local[0].wait()
    own.wait()
    pair[0].wait_recv()
    net_a, net_b, net_c = (Sender(near, *sems) for sems in ((send_a, recv_a), (send_b, recv_b), (send_c, recv_c)))
    ring = Gather(width, me, near, net_a, buf)
    line = [Gather(width, me, near, net, lines, (k,), 2) for k, net in ((0, net_b), (1, net_c))]
    ahead = Gather(width, me, near, net_b, quarter, (), 1)
    starts = [pltpu.make_async_copy(pack.at[0], view(buf, (slice(None),), CHIPS, me), line_sem.at[0, 0])]
    for k in range(2):
        for job, (mat, cols, order) in enumerate(jobs_of(width)):
            starts.append(pltpu.make_async_copy(pack.at[1 + k, mat, :, pl.ds(*cols)], line[k].block(job, 3), line_sem.at[1 + k, job]))
    for copy in starts:
        copy.start()
    save = pltpu.make_async_copy(pack.at[0], packed_out, loc_sem.at[4])
    save.start()
    for copy in starts:
        copy.wait()
    for part in [ring] + line:
        part.send(0)
    ring.forward(0)
    ring.finish(0)
    ring.send(1)
    for part in line:
        part.forward(0)
    ring.forward(1)
    ring.finish(1)
    ring.last_sends(full_out, store_sem)
    for part in line:
        part.finish(0)
    lines_save = [pltpu.make_async_copy(lines.at[k], out, loc_sem.at[9 + k]) for k, out in enumerate((line_out_0, line_out_1))]
    for copy in lines_save:
        copy.start()
    loads = ahead.load(lines.at[0], 2, quarter_sem)
    for copy in loads:
        copy.start()
    for copy in loads:
        copy.wait()
    ahead.send(1)
    for copy in local[1:]:
        copy.wait()
    for copy in pair[1:]:
        copy.wait_recv()
    outs = [pltpu.make_async_copy(x_val, x_out, loc_sem.at[6]), pltpu.make_async_copy(g_val, g_out, loc_sem.at[7])]
    for copy in outs:
        copy.start()
    ring.forward(2)
    ahead.forward(1)
    ahead.finish(1)
    outs.append(pltpu.make_async_copy(quarter, quarter_out, loc_sem.at[8]))
    outs[-1].start()
    ring.close_out(full_out, store_sem)
    for copy in outs + [save] + lines_save:
        copy.wait()
    for copy in pair:
        copy.wait_send()
    for net in (net_a, net_b, net_c):
        net.close()


def whole_of(width):
    return (4, SIDE, SIDE, SIDE, ROWS, width)


def open_call(up, down, x_loc, g_loc, call_id):
    tokens, width = x_loc.shape
    shape = lambda *dims: jax.ShapeDtypeStruct(dims, BF16)
    whole, quarter, line = whole_of(width), (4, SIDE, SIDE, ROWS, width), (4, SIDE, ROWS, width)
    vmem = lambda *dims: pltpu.VMEM(dims, BF16)
    sems = pltpu.SemaphoreType.DMA
    anywhere = pl.BlockSpec(memory_space=pl.ANY)
    return pl.pallas_call(
        functools.partial(open_kernel, width),
        out_shape=[shape(2 * tokens, width), shape(2 * tokens, width), shape(4, ROWS, width), shape(*whole), shape(*quarter), shape(*line), shape(*line)],
        in_specs=[pl.BlockSpec(memory_space=pltpu.VMEM)] + [anywhere] * 3,
        out_specs=[anywhere] * 7,
        scratch_shapes=[vmem(3, 2, 2, 8, width), vmem(3, 4, ROWS, width), vmem(2 * tokens, width), vmem(2 * tokens, width),
                        vmem(*whole), vmem(*quarter), vmem(2, *line)] + RING_SEMS * 3
        + [sems((11,)), sems((3,)), sems((3,)), sems((3, 6)), sems((6,)), sems((6, 4))],
        compiler_params=pltpu.CompilerParams(collective_id=call_id, has_side_effects=True, vmem_limit_bytes=VMEM_LIMIT),
        name="open",
    )(up, down.reshape(3, 2, ROWS, width), x_loc, g_loc)


def dot_nn(left, right):
    return lax.dot_general(left, right, (((1,), (0,)), ((), ())), preferred_element_type=F32)


def dot_nt(left, right):
    return lax.dot_general(left, right, (((1,), (1,)), ((), ())), preferred_element_type=F32)


def dot_tn(left, right):
    return lax.dot_general(left, right, (((0,), (0,)), ((), ())), preferred_element_type=F32)


def layer_kernel(forward, width, source, ahead, last_layer, *refs):
    refs = list(refs)
    take = lambda wanted: refs.pop(0) if wanted else None
    stream, weights, slope_in, begin, ahead_in = take(True), take(True), take(not forward), take(source), take(ahead)
    result, act_out, slope_out, next_out, ahead_out = take(True), take(True), take(forward), take(source), take(ahead)
    cur, mats, act, slope, part, got, pair_send, pair_recv, loc_sem, out_sem = refs[:10]
    tokens = cur.shape[0]
    tiles = tokens // TILE
    me, near = ring_places()
    core = lax.axis_index("c")
    partner = 1 - core
    loads = [pltpu.make_async_copy(stream, cur, loc_sem.at[0]), pltpu.make_async_copy(weights, mats, loc_sem.at[1])]
    if not forward:
        loads.append(pltpu.make_async_copy(slope_in, slope, loc_sem.at[2]))
    firsts = []
    if source:
        buf, send_sem, recv_sem, start_sem, store_sem = refs[10:15]
        net = Sender(near, send_sem, recv_sem)
        ring = Gather(width, me, near, net, buf)
        if source == "packed":
            firsts = [pltpu.make_async_copy(begin, view(buf, (slice(None),), CHIPS, me), start_sem.at[0])]
        else:
            firsts = ring.load(begin, 1 if source == "quarter" else 2, start_sem)
    if ahead:
        quarter, ahead_sem = refs[15:17]
        after = Gather(width, me, near, net, quarter, (), 1)
        firsts += after.load(ahead_in, 2, ahead_sem)
    for copy in firsts + loads:
        copy.start()
    enter(near, bool(source), partner)
    for copy in firsts:
        copy.wait()
    if ahead:
        after.send(1)
    if source == "packed":
        ring.through(0)
    if source in ("packed", "line"):
        ring.through(1)
    if source:
        ring.last_sends(next_out, store_sem)
    for copy in loads:
        copy.wait()

    def exchange(tile):
        rows = pl.ds(tile * TILE, TILE)
        return pltpu.make_async_remote_copy(
            src_ref=part.at[rows], dst_ref=got.at[rows], send_sem=pair_send.at[tile], recv_sem=pair_recv.at[tile],
            device_id={"c": partner}, device_id_type=MESH)

    def compute(tile, _):
        rows = pl.ds(pl.multiple_of(tile * TILE, TILE), TILE)
        left = cur[rows, :]
        for block in range(2):
            for cut in range(width // WIDE):
                cols = pl.ds(block * width + cut * WIDE, WIDE)
                if forward:
                    pre = dot_nn(left, mats[block * width:(block + 1) * width, cut * WIDE:(cut + 1) * WIDE])
                    act_val, slope_val = gelu_parts(pre)
                    act[rows, cols] = act_val.astype(BF16)
                    slope[rows, cols] = slope_val
                else:
                    low = (2 + block) * width + cut * WIDE
                    d_act = dot_nt(left, mats[low:low + WIDE, :])
                    act[rows, cols] = (d_act * slope[rows, cols]).astype(BF16)
        if forward:
            part[rows, :] = dot_nn(act[rows, :], mats[2 * width:, :])
        else:
            part[rows, :] = dot_nt(act[rows, :width], mats[:width, :]) + dot_nt(act[rows, width:], mats[width:2 * width, :])
        exchange(tile).start()
        return 0

    saves = []

    def save(k, low, high):
        rows = pl.ds(low * TILE, (high - low) * TILE)
        pairs = [(act, act_out)] + ([(slope, slope_out)] if forward else [])
        for n, (src, dst) in enumerate(pairs):
            saves.append(pltpu.make_async_copy(src.at[rows], dst.at[rows], out_sem.at[2 * k + n]))
            saves[-1].start()

    mid = tiles // 2
    lax.fori_loop(0, mid, compute, 0)
    save(0, 0, mid)
    if source:
        ring.forward(2)
    if ahead:
        after.forward(1)
    lax.fori_loop(mid, tiles, compute, 0)
    save(1, mid, tiles)
    for tile in range(tiles):
        exchange(tile).wait_recv()

    def total(rows):
        return (cur[rows, :].astype(F32) + (part[rows, :] + got[rows, :])).astype(BF16)

    if last_layer:
        for k in range(tiles // 2):
            rows = pl.ds(pl.multiple_of(core * (tokens // 2) + k * TILE, TILE), TILE)
            result[k * TILE:(k + 1) * TILE, :] = total(rows)
    else:
        for k in range(tiles):
            rows = pl.ds(k * TILE, TILE)
            result[rows, :] = total(rows)
    if ahead:
        after.finish(1)
        saves.append(pltpu.make_async_copy(quarter, ahead_out, out_sem.at[4]))
        saves[-1].start()
    if source:
        ring.close_out(next_out, store_sem)
        net.close()
    for copy in saves:
        copy.wait()
    for tile in range(tiles):
        exchange(tile).wait_send()


def layer_call(forward, stream, full, slope, call_id, source=None, begin=None, ahead=None, last_layer=False):
    tokens, width = stream.shape
    hidden = 2 * width
    shape = jax.ShapeDtypeStruct
    whole, quarter = whole_of(width), (4, SIDE, SIDE, ROWS, width)
    args = [stream, full.reshape(4 * width, width)] + ([] if forward else [slope])
    args += ([begin] if source else []) + ([] if ahead is None else [ahead])
    outs = [shape((tokens // 2 if last_layer else tokens, width), BF16), shape((tokens, hidden), BF16)]
    outs += [shape((tokens, hidden), F32)] if forward else []
    outs += ([shape(whole, BF16)] if source else []) + ([] if ahead is None else [shape(quarter, BF16)])
    tiles = tokens // TILE
    sems = pltpu.SemaphoreType.DMA
    scratch = [pltpu.VMEM((tokens, width), BF16), pltpu.VMEM((4 * width, width), BF16),
               pltpu.VMEM((tokens, hidden), BF16), pltpu.VMEM((tokens, hidden), F32),
               pltpu.VMEM((tokens, width), F32), pltpu.VMEM((tokens, width), F32),
               sems((tiles,)), sems((tiles,)), sems((4,)), sems((5,))]
    if source:
        scratch += [pltpu.VMEM(whole, BF16)] + RING_SEMS + [sems((6,)), sems((6, 4))]
    if ahead is not None:
        scratch += [pltpu.VMEM(quarter, BF16), sems((6,))]
    return pl.pallas_call(
        functools.partial(layer_kernel, forward, width, source, ahead is not None, last_layer),
        out_shape=outs,
        in_specs=[pl.BlockSpec(memory_space=pl.ANY)] * len(args),
        out_specs=[pl.BlockSpec(memory_space=pltpu.VMEM)] + [pl.BlockSpec(memory_space=pl.ANY)] * (len(outs) - 1),
        scratch_shapes=scratch,
        compiler_params=pltpu.CompilerParams(collective_id=call_id, has_side_effects=True, vmem_limit_bytes=VMEM_LIMIT),
        cost_estimate=pl.CostEstimate(flops=8 * tokens * hidden * width, bytes_accessed=40 << 20, transcendentals=0),
        name="forward_layer" if forward else "backward_layer",
    )(*args)


def add_into(dst, terms, lead):
    if not lead:
        dst[...] = sum((term[...] for term in terms), dst[...])
        return

    def step(k, _):
        add_into(dst.at[k], [term.at[k] for term in terms], lead[1:])
        return 0

    lax.fori_loop(0, lead[0], step, 0)


class RingSum:
    def __init__(self, width, me, near, buf, recv, send_sem, recv_sem):
        self.me, self.near, self.buf, self.recv, self.jobs = me, near, buf, recv, jobs_of(width)
        self.net = Sender(near, send_sem, recv_sem)

    def here(self, job, phase, d, part=None):
        mat, cols, order = self.jobs[job]
        sel = {a: self.me[a] for a in order[:phase]}
        sel[order[phase]] = self.near[order[phase]][d]
        if part is not None:
            sel.update(half(order[phase + 1], part))
        return view(self.buf, (mat,), CHIPS, sel, cols)

    def there(self, job, phase, slot, part=None):
        order = self.jobs[job][2]
        left = [a for a in CHIPS if a not in order[:phase + 1]]
        return view(self.recv[3 * job + phase], (slot,), left, {} if part is None else half(order[phase + 1], part))

    def lead(self, job, phase, part=None):
        order = self.jobs[job][2]
        return [2 if part is not None and a == order[phase + 1] else SIDE for a in CHIPS if a not in order[:phase + 1]]

    def push(self, job, phase, slot, d, part, to_slot, step):
        self.net.put((job, phase, slot), self.here(job, phase, d, part), self.there(job, phase, to_slot, part),
                     self.jobs[job][2][phase], step)

    def send(self, job, phase):
        if phase == 2:
            pieces = ((0, OPPOSITE, FULL, 0, NEXT), (3, PREV, FULL, 2, PREV))
        else:
            pieces = ((0, OPPOSITE, 0, 0, NEXT), (1, OPPOSITE, 1, 0, PREV), (2, NEXT, 1, 1, NEXT), (3, PREV, 0, 2, PREV))
        for slot, d, part, to_slot, step in pieces:
            self.push(job, phase, slot, d, part, to_slot, step)

    def pass_on(self, job, phase, arrived, slot, d, part, to_slot):
        self.net.got((job, phase, arrived))
        add_into(self.here(job, phase, d, part), [self.there(job, phase, 0, part)], self.lead(job, phase, part))
        self.push(job, phase, slot, d, part, to_slot, d)

    def mid(self, job, phase):
        if phase == 2:
            self.pass_on(job, phase, 0, 2, NEXT, FULL, 1)
        else:
            self.pass_on(job, phase, 0, 4, NEXT, 0, 1)
            self.pass_on(job, phase, 1, 5, PREV, 1, 2)

    def finish(self, job, phase):
        for slot in ((2, 3) if phase == 2 else (2, 3, 4, 5)):
            self.net.got((job, phase, slot))
        add_into(self.here(job, phase, HERE), [self.there(job, phase, slot) for slot in (1, 2)], self.lead(job, phase))


def recv_blocks(width):
    blocks = []
    for mat, cols, order in jobs_of(width):
        blocks += [pltpu.VMEM((3,) + (SIDE,) * (2 - phase) + (ROWS, cols[1]), F32) for phase in range(3)]
    return blocks


def sum_kernel(width, x_ref, act_ref, d_pre_ref, g_ref, up_out, down_out, x_val, act_val, d_pre, g_val, buf, *rest):
    send_sem, recv_sem, loc_sem, theirs, wide, pair_send, pair_recv = rest[18:]
    me, near = ring_places()
    core = lax.axis_index("c")
    ring = RingSum(width, me, near, buf, rest[:18], send_sem, recv_sem)
    upper, lower = pl.ds(0, width), pl.ds(width, width)
    loads = [pltpu.make_async_copy(src, dst, loc_sem.at[k]) for k, (src, dst) in enumerate(
        ((g_ref, g_val), (act_ref.at[:, lower], act_val.at[:, lower]), (act_ref.at[:, upper], act_val.at[:, upper]),
         (x_ref, x_val), (d_pre_ref, d_pre)))]
    for copy in loads:
        copy.start()
    enter(near, True, 1 - core)

    def grad(mat):
        def slab(z, _):
            if mat < 2:
                cols = pl.ds(pl.multiple_of(z * (width // SIDE), width // SIDE), width // SIDE)
                val = dot_tn(x_val[:, cols], d_pre[:, mat * width:(mat + 1) * width])
            else:
                cols = pl.ds(pl.multiple_of((mat - 2) * width + z * (width // SIDE), width // SIDE), width // SIDE)
                val = dot_tn(act_val[:, cols], g_val[...])
            buf[mat, z] = val.reshape(SIDE, SIDE, ROWS, width)
            return 0

        lax.fori_loop(0, SIDE, slab, 0)

    for copy in loads[:2]:
        copy.wait()
    grad(3)
    for job in SMALL:
        ring.send(job, 0)
    for copy in loads[2:]:
        copy.wait()
    for mat in (2, 0, 1):
        grad(mat)
        ring.send(LARGE[mat], 0)
        if mat == 0:
            for job in SMALL:
                ring.mid(job, 0)
    for job in LARGE:
        ring.mid(job, 0)
    for phase in range(3):
        for group in (SMALL, LARGE):
            for job in group:
                ring.finish(job, phase)
                if phase < 2:
                    ring.send(job, phase + 1)
        if phase < 2:
            for group in (SMALL, LARGE):
                for job in group:
                    ring.mid(job, phase + 1)
    own = [view(buf, (mat,), CHIPS, me) for mat in range(4)]
    pair = [pltpu.make_async_remote_copy(
        src_ref=own[mat].at[pl.ds(pl.multiple_of(8 * (1 - core), 8), 8)], dst_ref=theirs.at[mat], send_sem=pair_send.at[mat],
        recv_sem=pair_recv.at[mat], device_id={"c": 1 - core}, device_id_type=MESH) for mat in range(2)]
    for copy in pair:
        copy.start()
    for mat in (2, 3):
        down_out[(mat - 2) * ROWS:(mat - 1) * ROWS, :] = own[mat][...]
    places = column_places(512, 512)
    for copy in pair:
        copy.wait_recv()
    kept = pl.ds(pl.multiple_of(8 * core, 8), 8)
    for mat in range(2):
        first, second = own[mat][kept, :], theirs[mat]
        low, high = jnp.where(core == 0, first, second), jnp.where(core == 0, second, first)
        for group in range(width // 128):
            rows, cols = slice(8 * group, 8 * group + 8), slice(128 * group, 128 * group + 128)
            wide[rows, 128 * mat:128 * mat + 128] = low[:, cols]
            wide[rows, 256 + 128 * mat:384 + 128 * mat] = high[:, cols]
    rest_val = wide[...]
    total = None
    for _ in range(3):
        piece = rest_val.astype(BF16)
        rest_val = rest_val - piece.astype(F32)
        term = dot_nt(piece, places)
        total = term if total is None else total + term
    for group in range(width // 128):
        up_out[:, 512 * group:512 * group + 512] = total[8 * group:8 * group + 8, :]
    for copy in pair:
        copy.wait_send()
    ring.net.close()


def scatter_sum(x_in, act, d_pre, g_in, call_id):
    tokens, width = x_in.shape
    return pl.pallas_call(
        functools.partial(sum_kernel, width),
        out_shape=[jax.ShapeDtypeStruct((8, 4 * width), F32), jax.ShapeDtypeStruct((2 * ROWS, width), F32)],
        in_specs=[pl.BlockSpec(memory_space=pl.ANY)] * 4,
        out_specs=[pl.BlockSpec(memory_space=pltpu.VMEM)] * 2,
        scratch_shapes=[pltpu.VMEM((tokens, width), BF16), pltpu.VMEM((tokens, 2 * width), BF16),
                        pltpu.VMEM((tokens, 2 * width), BF16), pltpu.VMEM((tokens, width), BF16),
                        pltpu.VMEM((4, SIDE, SIDE, SIDE, ROWS, width), F32)] + recv_blocks(width)
        + RING_SEMS + [pltpu.SemaphoreType.DMA((5,)), pltpu.VMEM((2, 8, width), F32), pltpu.VMEM((8 * (width // 128), 512), F32),
                       pltpu.SemaphoreType.DMA((2,)), pltpu.SemaphoreType.DMA((2,))],
        compiler_params=pltpu.CompilerParams(collective_id=call_id, has_side_effects=True, vmem_limit_bytes=VMEM_LIMIT),
        cost_estimate=pl.CostEstimate(flops=8 * tokens * width * width, bytes_accessed=12 << 20, transcendentals=0),
        name="scatter_sum",
    )(x_in, act, d_pre, g_in)


def solution(mesh):
    grid = Mesh(mesh.devices.reshape(SIDE, SIDE, SIDE, 2), ALL)
    tok_spec = P(ALL, None)
    weight_spec = P(None, ALL, None)

    def device_step(x_loc, up_loc, down_loc, g_loc):
        x_0, g_3, packed, full, quarter_1, line_1, line_2 = open_call(up_loc, down_loc, x_loc, g_loc, 0)
        x_1, act_0, slope_0, full, quarter_2 = layer_call(True, x_0, full, None, 1, "quarter", quarter_1, line_2)
        x_2, act_1, slope_1, full = layer_call(True, x_1, full, None, 2, "quarter", quarter_2)
        y_out, act_2, slope_2, full = layer_call(True, x_2, full, None, 3, "line", line_2, last_layer=True)
        g_2, d_pre_2, full = layer_call(False, g_3, full, slope_2, 4, "line", line_1)
        sum_2 = scatter_sum(x_2, act_2, d_pre_2, g_3, 5)
        g_1, d_pre_1, full = layer_call(False, g_2, full, slope_1, 6, "packed", packed)
        sum_1 = scatter_sum(x_1, act_1, d_pre_1, g_2, 7)
        grad_in, d_pre_0 = layer_call(False, g_1, full, slope_0, 8, last_layer=True)
        sum_0 = scatter_sum(x_0, act_0, d_pre_0, g_1, 9)
        grad_up, grad_down = (jnp.stack(parts) for parts in zip(sum_0, sum_1, sum_2, strict=True))
        return y_out, grad_in, grad_up, grad_down

    return jax.shard_map(device_step, mesh=grid, in_specs=(tok_spec, weight_spec, weight_spec, tok_spec),
                         out_specs=(tok_spec, tok_spec, weight_spec, weight_spec), check_vma=False)
```

```python
import functools
import math

import jax
import jax.numpy as jnp
from jax import lax
from jax.experimental import pallas as pl
from jax.experimental.pallas import tpu as pltpu
from jax.sharding import Mesh, PartitionSpec as P

CHIPS = ("z", "y", "x")
ALL = CHIPS + ("c",)
BF16 = jnp.bfloat16
F32 = jnp.float32
SIDE = 4
ROWS = 16
TILE = 256
WIDE = 512
INV_SQRT_2PI = (2.0 * math.pi) ** -0.5
VMEM_LIMIT = 63 * 1024 * 1024
MESH = pl.DeviceIdType.MESH
HERE, NEXT, OPPOSITE, PREV = range(4)
FULL = None
ORDERS = (("x", "y", "z"), ("y", "z", "x"), ("z", "x", "y"))


def gelu_parts(pre_act):
    norm_cdf = 0.5 * (1.0 + lax.erf(pre_act * (2.0 ** -0.5)))
    norm_pdf = jnp.exp(-0.5 * pre_act * pre_act) * INV_SQRT_2PI
    return pre_act * norm_cdf, norm_cdf + pre_act * norm_pdf


def jobs_of(width):
    tile = width // 8
    cuts = ((0, 3 * tile), (3 * tile, 3 * tile), (6 * tile, 2 * tile))
    return [(3, cuts[k], ORDERS[k]) for k in range(3)] + [(mat, (0, width), ORDERS[mat]) for mat in range(3)]


JOBS = range(6)
SMALL, LARGE = JOBS[:3], JOBS[3:]


def view(ref, lead, axes, sel, cols=None):
    mid = tuple(sel.get(a, slice(None)) for a in axes)
    last = (slice(None), pl.ds(*cols)) if cols is not None else ()
    return ref.at[lead + mid + last]


def half(axis, k):
    return {axis: pl.ds(2 * k, 2)}


def ring_places():
    me = {a: lax.axis_index(a) for a in CHIPS}
    near = {a: [lax.rem(me[a] + d, SIDE) for d in range(SIDE)] for a in CHIPS}
    return me, near


def enter(near, ring=True, partner=None):
    barrier = pltpu.get_barrier_semaphore()
    if ring:
        for axis in CHIPS:
            for d in (1, 3):
                pl.semaphore_signal(barrier, inc=1, device_id={axis: near[axis][d]}, device_id_type=MESH)
    if partner is not None:
        pl.semaphore_signal(barrier, inc=1, device_id={"c": partner}, device_id_type=MESH)
    pl.semaphore_wait(barrier, 6 * ring + (partner is not None))


class Sender:
    def __init__(self, near, send_sem, recv_sem):
        self.near, self.send_sem, self.recv_sem, self.open = near, send_sem, recv_sem, {}

    def put(self, key, src, dst, axis, step):
        copy = pltpu.make_async_remote_copy(
            src_ref=src, dst_ref=dst, send_sem=self.send_sem.at[key], recv_sem=self.recv_sem.at[key],
            device_id={axis: self.near[axis][step]}, device_id_type=MESH)
        copy.start()
        self.open[key] = copy

    def got(self, key):
        self.open[key].wait_recv()

    def close(self):
        for copy in self.open.values():
            copy.wait_send()


RING_SEMS = [pltpu.SemaphoreType.DMA((6, 3, 6)), pltpu.SemaphoreType.DMA((6, 3, 6))]


class Gather:
    def __init__(self, width, me, near, net, buf, lead=(), skip=0):
        self.me, self.near, self.net, self.buf, self.jobs = me, near, net, buf, jobs_of(width)
        self.lead, self.skip = lead, skip

    def block(self, job, fixed, more=None, ref=None, skip=None):
        mat, cols, order = self.jobs[job]
        skip = self.skip if skip is None else skip
        sel = {a: self.me[a] for a in order[:fixed]}
        sel.update(more or {})
        lead = self.lead if ref is None else ()
        return view(self.buf if ref is None else ref, lead + (mat,), [a for a in CHIPS if a not in order[:skip]], sel, cols)

    def push(self, job, phase, slot, d, part, step):
        order = self.jobs[job][2]
        axis = order[2 - phase]
        sel = {axis: self.near[axis][d]}
        if part is not None:
            sel.update(half(order[3 - phase], part))
        here = self.block(job, 2 - phase, sel)
        self.net.put((job, phase, slot), here, here, axis, step)

    def send(self, phase):
        halves = ((FULL, NEXT), (FULL, PREV)) if phase == 0 else ((0, NEXT), (1, PREV), (1, NEXT), (0, PREV))
        for job in JOBS:
            for slot, (part, step) in enumerate(halves):
                self.push(job, phase, slot, HERE, part, step)

    def forward(self, phase):
        for job in JOBS:
            self.net.got((job, phase, 0))
            if phase == 0:
                self.push(job, phase, 2, PREV, FULL, NEXT)
            else:
                self.push(job, phase, 4, PREV, 0, NEXT)
                self.net.got((job, phase, 1))
                self.push(job, phase, 5, NEXT, 1, PREV)

    def finish(self, phase):
        for job in JOBS:
            for slot in ((1, 2) if phase == 0 else (2, 3, 4, 5)):
                self.net.got((job, phase, slot))

    def through(self, phase):
        self.send(phase)
        self.forward(phase)
        self.finish(phase)

    def load(self, src, fixed, sems):
        return [pltpu.make_async_copy(self.block(job, fixed, ref=src, skip=fixed, more=None), self.block(job, fixed), sems.at[job])
                for job in JOBS]

    def store(self, out, d, sems):
        for job in JOBS:
            axis = self.jobs[job][2][0]
            sel = {axis: self.near[axis][d]}
            copy = pltpu.make_async_copy(self.block(job, 0, sel), self.block(job, 0, sel, ref=out), sems.at[job, d])
            copy.start()
            self.stores.append(copy)

    def last_sends(self, out, sems):
        self.stores = []
        self.send(2)
        self.store(out, HERE, sems)

    def close_out(self, out, sems):
        for slots, places in (((2, 3), (NEXT, PREV)), ((4, 5), (OPPOSITE,))):
            for job in JOBS:
                for slot in slots:
                    self.net.got((job, 2, slot))
            for d in places:
                self.store(out, d, sems)
        for copy in self.stores:
            copy.wait()


def column_places(rows, cols):
    src = lax.broadcasted_iota(jnp.int32, (rows, cols), 0)
    dst = lax.broadcasted_iota(jnp.int32, (rows, cols), 1)
    want = ((dst & 127) >> 4) * 64 + (dst >> 8) * 32 + ((dst >> 7) & 1) * 16 + (dst & 15)
    return jnp.where(src == want, 1.0, 0.0).astype(BF16)


def open_kernel(width, up, down, x_ref, g_ref, x_out, g_out, packed_out, full_out, quarter_out, line_out_0, line_out_1,
                perm, pack, x_val, g_val, buf, quarter, lines, send_a, recv_a, send_b, recv_b, send_c, recv_c,
                loc_sem, pair_send, pair_recv, line_sem, quarter_sem, store_sem):
    me, near = ring_places()
    core = lax.axis_index("c")
    tokens = x_ref.shape[0]
    mine = pl.ds(pl.multiple_of(core * tokens, tokens), tokens)
    rows = pl.ds(pl.multiple_of(core * 8, 8), 8)
    local = [pltpu.make_async_copy(down, pack.at[:, 2:4], loc_sem.at[0]),
             pltpu.make_async_copy(x_ref, x_val.at[mine], loc_sem.at[1]),
             pltpu.make_async_copy(g_ref, g_val.at[mine], loc_sem.at[2])]
    for copy in local:
        copy.start()
    enter(near, True, 1 - core)
    places = column_places(512, 512)
    flat = up[...].reshape(24, 4 * width)
    for group in range(4 * width // 512):
        moved = lax.dot_general(flat[:, group * 512:(group + 1) * 512], places, (((1,), (0,)), ((), ())),
                                preferred_element_type=F32).astype(BF16)
        for k in range(4):
            perm[:, k // 2, k % 2, :, group * 128:(group + 1) * 128] = moved[:, k * 128:(k + 1) * 128].reshape(3, 8, 128)
    pair = [pltpu.make_async_remote_copy(src_ref=src, dst_ref=dst, send_sem=pair_send.at[k], recv_sem=pair_recv.at[k],
                                         device_id={"c": 1 - core}, device_id_type=MESH)
            for k, (src, dst) in enumerate(((perm.at[:, 1 - core], pack.at[:, 0:2, rows]),
                                            (x_ref, x_val.at[mine]), (g_ref, g_val.at[mine])))]
    for copy in pair[1:]:
        copy.start()
    pair[0].start()
    own = pltpu.make_async_copy(perm.at[:, core], pack.at[:, 0:2, rows], loc_sem.at[3])
    own.start()
    local[0].wait()
    own.wait()
    pair[0].wait_recv()
    net_a, net_b, net_c = (Sender(near, *sems) for sems in ((send_a, recv_a), (send_b, recv_b), (send_c, recv_c)))
    ring = Gather(width, me, near, net_a, buf)
    line = [Gather(width, me, near, net, lines, (k,), 2) for k, net in ((0, net_b), (1, net_c))]
    ahead = Gather(width, me, near, net_b, quarter, (), 1)
    starts = [pltpu.make_async_copy(pack.at[0], view(buf, (slice(None),), CHIPS, me), line_sem.at[0, 0])]
    for k in range(2):
        for job, (mat, cols, order) in enumerate(jobs_of(width)):
            starts.append(pltpu.make_async_copy(pack.at[1 + k, mat, :, pl.ds(*cols)], line[k].block(job, 3), line_sem.at[1 + k, job]))
    for copy in starts:
        copy.start()
    save = pltpu.make_async_copy(pack.at[0], packed_out, loc_sem.at[4])
    save.start()
    for copy in starts:
        copy.wait()
    for part in [ring] + line:
        part.send(0)
    ring.forward(0)
    ring.finish(0)
    ring.send(1)
    for part in line:
        part.forward(0)
    ring.forward(1)
    ring.finish(1)
    ring.last_sends(full_out, store_sem)
    for part in line:
        part.finish(0)
    lines_save = [pltpu.make_async_copy(lines.at[k], out, loc_sem.at[9 + k]) for k, out in enumerate((line_out_0, line_out_1))]
    for copy in lines_save:
        copy.start()
    loads = ahead.load(lines.at[0], 2, quarter_sem)
    for copy in loads:
        copy.start()
    for copy in loads:
        copy.wait()
    ahead.send(1)
    for copy in local[1:]:
        copy.wait()
    for copy in pair[1:]:
        copy.wait_recv()
    outs = [pltpu.make_async_copy(x_val, x_out, loc_sem.at[6]), pltpu.make_async_copy(g_val, g_out, loc_sem.at[7])]
    for copy in outs:
        copy.start()
    ring.forward(2)
    ahead.forward(1)
    ahead.finish(1)
    outs.append(pltpu.make_async_copy(quarter, quarter_out, loc_sem.at[8]))
    outs[-1].start()
    ring.close_out(full_out, store_sem)
    for copy in outs + [save] + lines_save:
        copy.wait()
    for copy in pair:
        copy.wait_send()
    for net in (net_a, net_b, net_c):
        net.close()


def whole_of(width):
    return (4, SIDE, SIDE, SIDE, ROWS, width)


def open_call(up, down, x_loc, g_loc, call_id):
    tokens, width = x_loc.shape
    shape = lambda *dims: jax.ShapeDtypeStruct(dims, BF16)
    whole, quarter, line = whole_of(width), (4, SIDE, SIDE, ROWS, width), (4, SIDE, ROWS, width)
    vmem = lambda *dims: pltpu.VMEM(dims, BF16)
    sems = pltpu.SemaphoreType.DMA
    anywhere = pl.BlockSpec(memory_space=pl.ANY)
    return pl.pallas_call(
        functools.partial(open_kernel, width),
        out_shape=[shape(2 * tokens, width), shape(2 * tokens, width), shape(4, ROWS, width), shape(*whole), shape(*quarter), shape(*line), shape(*line)],
        in_specs=[pl.BlockSpec(memory_space=pltpu.VMEM)] + [anywhere] * 3,
        out_specs=[anywhere] * 7,
        scratch_shapes=[vmem(3, 2, 2, 8, width), vmem(3, 4, ROWS, width), vmem(2 * tokens, width), vmem(2 * tokens, width),
                        vmem(*whole), vmem(*quarter), vmem(2, *line)] + RING_SEMS * 3
        + [sems((11,)), sems((3,)), sems((3,)), sems((3, 6)), sems((6,)), sems((6, 4))],
        compiler_params=pltpu.CompilerParams(collective_id=call_id, has_side_effects=True, vmem_limit_bytes=VMEM_LIMIT),
        name="open",
    )(up, down.reshape(3, 2, ROWS, width), x_loc, g_loc)


def dot_nn(left, right):
    return lax.dot_general(left, right, (((1,), (0,)), ((), ())), preferred_element_type=F32)


def dot_nt(left, right):
    return lax.dot_general(left, right, (((1,), (1,)), ((), ())), preferred_element_type=F32)


def dot_tn(left, right):
    return lax.dot_general(left, right, (((0,), (0,)), ((), ())), preferred_element_type=F32)


def layer_kernel(forward, width, source, ahead, pre, last_layer, *refs):
    refs = list(refs)
    take = lambda wanted: refs.pop(0) if wanted else None
    stream, weights, slope_in, act_in = take(True), take(True), take(not forward), take(not forward)
    begin, ahead_in, pre_in = take(source), take(ahead), take(pre)
    result, act_out, slope_out, grad_out = take(True), take(True), take(forward), take(not forward)
    next_out, ahead_out, pre_out = take(source), take(ahead), take(pre)
    act_low, grad_low = (refs.pop(), refs.pop()) if not forward else (None, None)
    cur, mats, act, slope, part, got, pair_send, pair_recv, loc_sem, out_sem = refs[:10]
    tokens = cur.shape[0]
    tiles = tokens // TILE
    me, near = ring_places()
    core = lax.axis_index("c")
    partner = 1 - core
    loads = [pltpu.make_async_copy(stream, cur, loc_sem.at[0]), pltpu.make_async_copy(weights, mats, loc_sem.at[1])]
    if not forward:
        loads.append(pltpu.make_async_copy(slope_in, slope, loc_sem.at[2]))
        loads.append(pltpu.make_async_copy(act_in.at[:, pl.ds(width, width)], act_low, loc_sem.at[3]))
    firsts = []
    if source:
        buf, send_sem, recv_sem, start_sem, store_sem = refs[10:15]
        net = Sender(near, send_sem, recv_sem)
        ring = Gather(width, me, near, net, buf)
        firsts = ring.load(begin, 1 if source == "quarter" else 2, start_sem)
    if ahead:
        quarter, ahead_sem = refs[15:17]
        after = Gather(width, me, near, net, quarter, (), 1)
        firsts += after.load(ahead_in, 2, ahead_sem)
    if pre:
        line, pre_sem = refs[15:17]
        before = Gather(width, me, near, net, line, (), 2)
        firsts += [pltpu.make_async_copy(pre_in.at[mat, :, pl.ds(*cols)], before.block(job, 3), pre_sem.at[job])
                   for job, (mat, cols, order) in enumerate(before.jobs)]
    for copy in firsts + loads:
        copy.start()
    enter(near, bool(source), partner)
    for copy in firsts:
        copy.wait()
    if ahead:
        after.send(1)
    if pre:
        before.send(0)
    if source == "line":
        ring.through(1)
    if source:
        ring.last_sends(next_out, store_sem)
    for copy in loads:
        copy.wait()

    def exchange(tile):
        rows = pl.ds(tile * TILE, TILE)
        return pltpu.make_async_remote_copy(
            src_ref=part.at[rows], dst_ref=got.at[rows], send_sem=pair_send.at[tile], recv_sem=pair_recv.at[tile],
            device_id={"c": partner}, device_id_type=MESH)

    def compute(tile, _):
        rows = pl.ds(pl.multiple_of(tile * TILE, TILE), TILE)
        left = cur[rows, :]
        for block in range(2):
            for cut in range(width // WIDE):
                cols = pl.ds(block * width + cut * WIDE, WIDE)
                if forward:
                    pre = dot_nn(left, mats[block * width:(block + 1) * width, cut * WIDE:(cut + 1) * WIDE])
                    act_val, slope_val = gelu_parts(pre)
                    act[rows, cols] = act_val.astype(BF16)
                    slope[rows, cols] = slope_val
                else:
                    low = (2 + block) * width + cut * WIDE
                    d_act = dot_nt(left, mats[low:low + WIDE, :])
                    act[rows, cols] = (d_act * slope[rows, cols]).astype(BF16)
        if forward:
            part[rows, :] = dot_nn(act[rows, :], mats[2 * width:, :])
        else:
            part[rows, :] = dot_nt(act[rows, :width], mats[:width, :]) + dot_nt(act[rows, width:], mats[width:2 * width, :])
        exchange(tile).start()
        return 0

    def low_slab(z, _):
        slab = width // SIDE
        val = dot_tn(act_low[:, pl.ds(pl.multiple_of(z * slab, slab), slab)], cur[...])
        grad_low[z] = val.reshape(SIDE, SIDE, ROWS, width)
        return 0

    saves = []

    def save(k, low, high):
        rows = pl.ds(low * TILE, (high - low) * TILE)
        pairs = [(act, act_out)] + ([(slope, slope_out)] if forward else [])
        for n, (src, dst) in enumerate(pairs):
            saves.append(pltpu.make_async_copy(src.at[rows], dst.at[rows], out_sem.at[2 * k + n]))
            saves[-1].start()

    mid = tiles // 2
    lax.fori_loop(0, mid, compute, 0)
    save(0, 0, mid)
    if source:
        ring.forward(2)
    if ahead:
        after.forward(1)
    if pre:
        before.forward(0)
    if not forward:
        lax.fori_loop(0, SIDE, low_slab, 0)
        saves.append(pltpu.make_async_copy(grad_low, grad_out, out_sem.at[1]))
        saves[-1].start()
    lax.fori_loop(mid, tiles, compute, 0)
    save(1, mid, tiles)
    for tile in range(tiles):
        exchange(tile).wait_recv()

    def total(rows):
        return (cur[rows, :].astype(F32) + (part[rows, :] + got[rows, :])).astype(BF16)

    if last_layer:
        for k in range(tiles // 2):
            rows = pl.ds(pl.multiple_of(core * (tokens // 2) + k * TILE, TILE), TILE)
            result[k * TILE:(k + 1) * TILE, :] = total(rows)
    else:
        for k in range(tiles):
            rows = pl.ds(k * TILE, TILE)
            result[rows, :] = total(rows)
    if ahead:
        after.finish(1)
        saves.append(pltpu.make_async_copy(quarter, ahead_out, out_sem.at[4]))
        saves[-1].start()
    if pre:
        before.finish(0)
        saves.append(pltpu.make_async_copy(line, pre_out, out_sem.at[4]))
        saves[-1].start()
    if source:
        ring.close_out(next_out, store_sem)
        net.close()
    for copy in saves:
        copy.wait()
    for tile in range(tiles):
        exchange(tile).wait_send()


def layer_call(forward, stream, full, kept, call_id, source=None, begin=None, ahead=None, pre=None, last_layer=False):
    tokens, width = stream.shape
    hidden = 2 * width
    shape = jax.ShapeDtypeStruct
    whole, quarter = whole_of(width), (4, SIDE, SIDE, ROWS, width)
    args = [stream, full.reshape(4 * width, width)] + ([] if forward else list(kept))
    args += [val for val in (begin, ahead, pre) if val is not None]
    outs = [shape((tokens // 2 if last_layer else tokens, width), BF16), shape((tokens, hidden), BF16)]
    outs += [shape((tokens, hidden), F32) if forward else shape(whole[1:], F32)]
    outs += ([shape(whole, BF16)] if source else []) + ([] if ahead is None else [shape(quarter, BF16)])
    outs += [] if pre is None else [shape(quarter[1:], BF16)]
    tiles = tokens // TILE
    sems = pltpu.SemaphoreType.DMA
    scratch = [pltpu.VMEM((tokens, width), BF16), pltpu.VMEM((4 * width, width), BF16),
               pltpu.VMEM((tokens, hidden), BF16), pltpu.VMEM((tokens, hidden), F32),
               pltpu.VMEM((tokens, width), F32), pltpu.VMEM((tokens, width), F32),
               sems((tiles,)), sems((tiles,)), sems((4,)), sems((5,))]
    if source:
        scratch += [pltpu.VMEM(whole, BF16)] + RING_SEMS + [sems((6,)), sems((6, 4))]
    if ahead is not None:
        scratch += [pltpu.VMEM(quarter, BF16), sems((6,))]
    if pre is not None:
        scratch += [pltpu.VMEM(quarter[1:], BF16), sems((6,))]
    if not forward:
        scratch += [pltpu.VMEM(whole[1:], F32), pltpu.VMEM((tokens, width), BF16)]
    return pl.pallas_call(
        functools.partial(layer_kernel, forward, width, source, ahead is not None, pre is not None, last_layer),
        out_shape=outs,
        in_specs=[pl.BlockSpec(memory_space=pl.ANY)] * len(args),
        out_specs=[pl.BlockSpec(memory_space=pltpu.VMEM)] + [pl.BlockSpec(memory_space=pl.ANY)] * (len(outs) - 1),
        scratch_shapes=scratch,
        compiler_params=pltpu.CompilerParams(collective_id=call_id, has_side_effects=True, vmem_limit_bytes=VMEM_LIMIT),
        cost_estimate=pl.CostEstimate(flops=8 * tokens * hidden * width, bytes_accessed=40 << 20, transcendentals=0),
        name="forward_layer" if forward else "backward_layer",
    )(*args)


def add_into(dst, terms, lead):
    if not lead:
        dst[...] = sum((term[...] for term in terms), dst[...])
        return

    def step(k, _):
        add_into(dst.at[k], [term.at[k] for term in terms], lead[1:])
        return 0

    lax.fori_loop(0, lead[0], step, 0)


class RingSum:
    def __init__(self, width, me, near, buf, recv, send_sem, recv_sem):
        self.me, self.near, self.buf, self.recv, self.jobs = me, near, buf, recv, jobs_of(width)
        self.net = Sender(near, send_sem, recv_sem)

    def here(self, job, phase, d, part=None):
        mat, cols, order = self.jobs[job]
        sel = {a: self.me[a] for a in order[:phase]}
        sel[order[phase]] = self.near[order[phase]][d]
        if part is not None:
            sel.update(half(order[phase + 1], part))
        return view(self.buf, (mat,), CHIPS, sel, cols)

    def there(self, job, phase, slot, part=None):
        order = self.jobs[job][2]
        left = [a for a in CHIPS if a not in order[:phase + 1]]
        return view(self.recv[3 * job + phase], (slot,), left, {} if part is None else half(order[phase + 1], part))

    def lead(self, job, phase, part=None):
        order = self.jobs[job][2]
        return [2 if part is not None and a == order[phase + 1] else SIDE for a in CHIPS if a not in order[:phase + 1]]

    def push(self, job, phase, slot, d, part, to_slot, step):
        self.net.put((job, phase, slot), self.here(job, phase, d, part), self.there(job, phase, to_slot, part),
                     self.jobs[job][2][phase], step)

    def send(self, job, phase):
        if phase == 2:
            pieces = ((0, OPPOSITE, FULL, 0, NEXT), (3, PREV, FULL, 2, PREV))
        else:
            pieces = ((0, OPPOSITE, 0, 0, NEXT), (1, OPPOSITE, 1, 0, PREV), (2, NEXT, 1, 1, NEXT), (3, PREV, 0, 2, PREV))
        for slot, d, part, to_slot, step in pieces:
            self.push(job, phase, slot, d, part, to_slot, step)

    def pass_on(self, job, phase, arrived, slot, d, part, to_slot):
        self.net.got((job, phase, arrived))
        add_into(self.here(job, phase, d, part), [self.there(job, phase, 0, part)], self.lead(job, phase, part))
        self.push(job, phase, slot, d, part, to_slot, d)

    def mid(self, job, phase):
        if phase == 2:
            self.pass_on(job, phase, 0, 2, NEXT, FULL, 1)
        else:
            self.pass_on(job, phase, 0, 4, NEXT, 0, 1)
            self.pass_on(job, phase, 1, 5, PREV, 1, 2)

    def finish(self, job, phase):
        for slot in ((2, 3) if phase == 2 else (2, 3, 4, 5)):
            self.net.got((job, phase, slot))
        add_into(self.here(job, phase, HERE), [self.there(job, phase, slot) for slot in (1, 2)], self.lead(job, phase))


def recv_blocks(width):
    blocks = []
    for mat, cols, order in jobs_of(width):
        blocks += [pltpu.VMEM((3,) + (SIDE,) * (2 - phase) + (ROWS, cols[1]), F32) for phase in range(3)]
    return blocks


def sum_kernel(width, x_ref, act_ref, d_pre_ref, g_ref, low_ref, up_out, down_out, x_val, act_val, d_pre, g_val, buf, *rest):
    send_sem, recv_sem, loc_sem, theirs, wide, pair_send, pair_recv, low_sem = rest[18:]
    me, near = ring_places()
    core = lax.axis_index("c")
    ring = RingSum(width, me, near, buf, rest[:18], send_sem, recv_sem)
    low = {}
    for d in (OPPOSITE, NEXT, PREV, HERE):
        for job in SMALL:
            mat, cols, order = ring.jobs[job]
            src = view(low_ref, (), CHIPS, {order[0]: near[order[0]][d]}, cols)
            low[job, d] = pltpu.make_async_copy(src, ring.here(job, 0, d), low_sem.at[job, d])
            low[job, d].start()
    loads = [pltpu.make_async_copy(src, dst, loc_sem.at[k]) for k, (src, dst) in enumerate(
        ((g_ref, g_val), (act_ref.at[:, pl.ds(0, width)], act_val), (x_ref, x_val), (d_pre_ref, d_pre)))]
    for copy in loads:
        copy.start()
    enter(near, True, 1 - core)

    def grad(mat):
        def slab(z, _):
            if mat < 2:
                cols = pl.ds(pl.multiple_of(z * (width // SIDE), width // SIDE), width // SIDE)
                val = dot_tn(x_val[:, cols], d_pre[:, mat * width:(mat + 1) * width])
            else:
                cols = pl.ds(pl.multiple_of(z * (width // SIDE), width // SIDE), width // SIDE)
                val = dot_tn(act_val[:, cols], g_val[...])
            buf[mat, z] = val.reshape(SIDE, SIDE, ROWS, width)
            return 0

        lax.fori_loop(0, SIDE, slab, 0)

    for job in SMALL:
        for d in (OPPOSITE, NEXT, PREV):
            low[job, d].wait()
        ring.send(job, 0)
    for copy in loads:
        copy.wait()
    for mat in (2, 0, 1):
        grad(mat)
        ring.send(LARGE[mat], 0)
        if mat == 0:
            for job in SMALL:
                ring.mid(job, 0)
    for job in LARGE:
        ring.mid(job, 0)
    for job in SMALL:
        low[job, HERE].wait()
    for phase in range(3):
        for group in (SMALL, LARGE):
            for job in group:
                ring.finish(job, phase)
                if phase < 2:
                    ring.send(job, phase + 1)
        if phase < 2:
            for group in (SMALL, LARGE):
                for job in group:
                    ring.mid(job, phase + 1)
    own = [view(buf, (mat,), CHIPS, me) for mat in range(4)]
    pair = [pltpu.make_async_remote_copy(
        src_ref=own[mat].at[pl.ds(pl.multiple_of(8 * (1 - core), 8), 8)], dst_ref=theirs.at[mat], send_sem=pair_send.at[mat],
        recv_sem=pair_recv.at[mat], device_id={"c": 1 - core}, device_id_type=MESH) for mat in range(2)]
    for copy in pair:
        copy.start()
    for mat in (2, 3):
        down_out[(mat - 2) * ROWS:(mat - 1) * ROWS, :] = own[mat][...]
    places = column_places(512, 512)
    for copy in pair:
        copy.wait_recv()
    kept = pl.ds(pl.multiple_of(8 * core, 8), 8)
    for mat in range(2):
        first, second = own[mat][kept, :], theirs[mat]
        low, high = jnp.where(core == 0, first, second), jnp.where(core == 0, second, first)
        for group in range(width // 128):
            rows, cols = slice(8 * group, 8 * group + 8), slice(128 * group, 128 * group + 128)
            wide[rows, 128 * mat:128 * mat + 128] = low[:, cols]
            wide[rows, 256 + 128 * mat:384 + 128 * mat] = high[:, cols]
    rest_val = wide[...]
    total = None
    for _ in range(3):
        piece = rest_val.astype(BF16)
        rest_val = rest_val - piece.astype(F32)
        term = dot_nt(piece, places)
        total = term if total is None else total + term
    for group in range(width // 128):
        up_out[:, 512 * group:512 * group + 512] = total[8 * group:8 * group + 8, :]
    for copy in pair:
        copy.wait_send()
    ring.net.close()


def scatter_sum(x_in, act, d_pre, g_in, low, call_id):
    tokens, width = x_in.shape
    return pl.pallas_call(
        functools.partial(sum_kernel, width),
        out_shape=[jax.ShapeDtypeStruct((8, 4 * width), F32), jax.ShapeDtypeStruct((2 * ROWS, width), F32)],
        in_specs=[pl.BlockSpec(memory_space=pl.ANY)] * 5,
        out_specs=[pl.BlockSpec(memory_space=pltpu.VMEM)] * 2,
        scratch_shapes=[pltpu.VMEM((tokens, width), BF16), pltpu.VMEM((tokens, width), BF16),
                        pltpu.VMEM((tokens, 2 * width), BF16), pltpu.VMEM((tokens, width), BF16),
                        pltpu.VMEM((4, SIDE, SIDE, SIDE, ROWS, width), F32)] + recv_blocks(width)
        + RING_SEMS + [pltpu.SemaphoreType.DMA((5,)), pltpu.VMEM((2, 8, width), F32), pltpu.VMEM((8 * (width // 128), 512), F32),
                       pltpu.SemaphoreType.DMA((2,)), pltpu.SemaphoreType.DMA((2,)), pltpu.SemaphoreType.DMA((3, 4))],
        compiler_params=pltpu.CompilerParams(collective_id=call_id, has_side_effects=True, vmem_limit_bytes=VMEM_LIMIT),
        cost_estimate=pl.CostEstimate(flops=8 * tokens * width * width, bytes_accessed=12 << 20, transcendentals=0),
        name="scatter_sum",
    )(x_in, act, d_pre, g_in, low)


def solution(mesh):
    grid = Mesh(mesh.devices.reshape(SIDE, SIDE, SIDE, 2), ALL)
    tok_spec = P(ALL, None)
    weight_spec = P(None, ALL, None)

    def device_step(x_loc, up_loc, down_loc, g_loc):
        x_0, g_3, packed, full, quarter_1, line_1, line_2 = open_call(up_loc, down_loc, x_loc, g_loc, 0)
        x_1, act_0, slope_0, full, quarter_2 = layer_call(True, x_0, full, None, 1, "quarter", quarter_1, line_2)
        x_2, act_1, slope_1, full = layer_call(True, x_1, full, None, 2, "quarter", quarter_2)
        y_out, act_2, slope_2, full = layer_call(True, x_2, full, None, 3, "line", line_2, last_layer=True)
        g_2, d_pre_2, low_2, full, line_0 = layer_call(False, g_3, full, (slope_2, act_2), 4, "line", line_1, pre=packed)
        sum_2 = scatter_sum(x_2, act_2, d_pre_2, g_3, low_2, 5)
        g_1, d_pre_1, low_1, full = layer_call(False, g_2, full, (slope_1, act_1), 6, "line", line_0)
        sum_1 = scatter_sum(x_1, act_1, d_pre_1, g_2, low_1, 7)
        grad_in, d_pre_0, low_0 = layer_call(False, g_1, full, (slope_0, act_0), 8, last_layer=True)
        sum_0 = scatter_sum(x_0, act_0, d_pre_0, g_1, low_0, 9)
        grad_up, grad_down = (jnp.stack(parts) for parts in zip(sum_0, sum_1, sum_2, strict=True))
        return y_out, grad_in, grad_up, grad_down

    return jax.shard_map(device_step, mesh=grid, in_specs=(tok_spec, weight_spec, weight_spec, tok_spec),
                         out_specs=(tok_spec, tok_spec, weight_spec, weight_spec), check_vma=False)
```

```python
import functools
import itertools
import math

import jax
import jax.numpy as jnp
from jax import lax
from jax.experimental import pallas as pl
from jax.experimental.pallas import tpu as pltpu
from jax.sharding import Mesh, PartitionSpec as P

CHIPS = ("z", "y", "x")
ALL = CHIPS + ("c",)
BF16 = jnp.bfloat16
F32 = jnp.float32
SIDE = 4
ROWS = 16
TILE = 256
WIDE = 512
INV_SQRT_2PI = (2.0 * math.pi) ** -0.5
VMEM_LIMIT = 63 * 1024 * 1024
MESH = pl.DeviceIdType.MESH
HERE, NEXT, OPPOSITE, PREV = range(4)
FULL = None
ORDERS = (("x", "y", "z"), ("y", "z", "x"), ("z", "x", "y"))


def gelu_parts(pre_act):
    norm_cdf = 0.5 * (1.0 + lax.erf(pre_act * (2.0 ** -0.5)))
    norm_pdf = jnp.exp(-0.5 * pre_act * pre_act) * INV_SQRT_2PI
    return pre_act * norm_cdf, norm_cdf + pre_act * norm_pdf


def jobs_of(width):
    tile = width // 8
    cuts = ((0, 3 * tile), (3 * tile, 3 * tile), (6 * tile, 2 * tile))
    return [(3, cuts[k], ORDERS[k]) for k in range(3)] + [(mat, (0, width), ORDERS[mat]) for mat in range(3)]


JOBS = range(6)
SMALL, LARGE = JOBS[:3], JOBS[3:]


def view(ref, lead, axes, sel, cols=None):
    mid = tuple(sel.get(a, slice(None)) for a in axes)
    last = (slice(None), pl.ds(*cols)) if cols is not None else ()
    return ref.at[lead + mid + last]


def half(axis, k):
    return {axis: pl.ds(2 * k, 2)}


def ring_places():
    me = {a: lax.axis_index(a) for a in CHIPS}
    near = {a: [lax.rem(me[a] + d, SIDE) for d in range(SIDE)] for a in CHIPS}
    return me, near


def enter(near, ring=True, partner=None):
    barrier = pltpu.get_barrier_semaphore()
    if ring:
        for axis in CHIPS:
            for d in (1, 3):
                pl.semaphore_signal(barrier, inc=1, device_id={axis: near[axis][d]}, device_id_type=MESH)
    if partner is not None:
        pl.semaphore_signal(barrier, inc=1, device_id={"c": partner}, device_id_type=MESH)
    pl.semaphore_wait(barrier, 6 * ring + (partner is not None))


class Sender:
    def __init__(self, near, send_sem, recv_sem):
        self.near, self.send_sem, self.recv_sem, self.open = near, send_sem, recv_sem, {}

    def put(self, key, src, dst, axis, step):
        copy = pltpu.make_async_remote_copy(
            src_ref=src, dst_ref=dst, send_sem=self.send_sem.at[key], recv_sem=self.recv_sem.at[key],
            device_id={axis: self.near[axis][step]}, device_id_type=MESH)
        copy.start()
        self.open[key] = copy

    def got(self, key):
        self.open[key].wait_recv()

    def close(self):
        for copy in self.open.values():
            copy.wait_send()


RING_SEMS = [pltpu.SemaphoreType.DMA((6, 3, 6)), pltpu.SemaphoreType.DMA((6, 3, 6))]


class Gather:
    def __init__(self, width, me, near, net, buf, lead=(), skip=0):
        self.me, self.near, self.net, self.buf, self.jobs = me, near, net, buf, jobs_of(width)
        self.lead, self.skip = lead, skip

    def block(self, job, fixed, more=None, ref=None, skip=None):
        mat, cols, order = self.jobs[job]
        skip = self.skip if skip is None else skip
        sel = {a: self.me[a] for a in order[:fixed]}
        sel.update(more or {})
        lead = self.lead if ref is None else ()
        return view(self.buf if ref is None else ref, lead + (mat,), [a for a in CHIPS if a not in order[:skip]], sel, cols)

    def push(self, job, phase, slot, d, part, step):
        order = self.jobs[job][2]
        axis = order[2 - phase]
        sel = {axis: self.near[axis][d]}
        if part is not None:
            sel.update(half(order[3 - phase], part))
        here = self.block(job, 2 - phase, sel)
        self.net.put((job, phase, slot), here, here, axis, step)

    def send(self, phase):
        halves = ((FULL, NEXT), (FULL, PREV)) if phase == 0 else ((0, NEXT), (1, PREV), (1, NEXT), (0, PREV))
        for job in JOBS:
            for slot, (part, step) in enumerate(halves):
                self.push(job, phase, slot, HERE, part, step)

    def forward(self, phase):
        for job in JOBS:
            self.net.got((job, phase, 0))
            if phase == 0:
                self.push(job, phase, 2, PREV, FULL, NEXT)
            else:
                self.push(job, phase, 4, PREV, 0, NEXT)
                self.net.got((job, phase, 1))
                self.push(job, phase, 5, NEXT, 1, PREV)

    def finish(self, phase):
        for job in JOBS:
            for slot in ((1, 2) if phase == 0 else (2, 3, 4, 5)):
                self.net.got((job, phase, slot))

    def load(self, src, fixed, sems):
        return [pltpu.make_async_copy(self.block(job, fixed, ref=src, skip=fixed), self.block(job, fixed), sems.at[job])
                for job in JOBS]

    def store(self, out, d, sems):
        for job in JOBS:
            axis = self.jobs[job][2][0]
            sel = {axis: self.near[axis][d]}
            copy = pltpu.make_async_copy(self.block(job, 0, sel), self.block(job, 0, sel, ref=out), sems.at[job, d])
            copy.start()
            self.stores.append(copy)

    def last_sends(self, out, sems):
        self.stores = []
        self.send(2)
        self.store(out, HERE, sems)

    def close_out(self, out, sems):
        for slots, places in (((2, 3), (NEXT, PREV)), ((4, 5), (OPPOSITE,))):
            for job in JOBS:
                for slot in slots:
                    self.net.got((job, 2, slot))
            for d in places:
                self.store(out, d, sems)
        for copy in self.stores:
            copy.wait()


def column_places(rows, cols):
    src = lax.broadcasted_iota(jnp.int32, (rows, cols), 0)
    dst = lax.broadcasted_iota(jnp.int32, (rows, cols), 1)
    want = ((dst & 127) >> 4) * 64 + (dst >> 8) * 32 + ((dst >> 7) & 1) * 16 + (dst & 15)
    return jnp.where(src == want, 1.0, 0.0).astype(BF16)


def open_kernel(width, up, down, x_ref, g_ref, x_out, g_out, packed_out, full_out, quarter_out, line_out_0, line_out_1,
                perm, pack, x_val, g_val, buf, quarter, lines, send_a, recv_a, send_b, recv_b, send_c, recv_c,
                loc_sem, pair_send, pair_recv, line_sem, quarter_sem, store_sem):
    me, near = ring_places()
    core = lax.axis_index("c")
    tokens = x_ref.shape[0]
    mine = pl.ds(pl.multiple_of(core * tokens, tokens), tokens)
    rows = pl.ds(pl.multiple_of(core * 8, 8), 8)
    local = [pltpu.make_async_copy(down, pack.at[:, 2:4], loc_sem.at[0]),
             pltpu.make_async_copy(x_ref, x_val.at[mine], loc_sem.at[1]),
             pltpu.make_async_copy(g_ref, g_val.at[mine], loc_sem.at[2])]
    for copy in local:
        copy.start()
    enter(near, True, 1 - core)
    places = column_places(512, 512)
    flat = up[...].reshape(24, 4 * width)
    for group in range(4 * width // 512):
        moved = lax.dot_general(flat[:, group * 512:(group + 1) * 512], places, (((1,), (0,)), ((), ())),
                                preferred_element_type=F32).astype(BF16)
        for k in range(4):
            perm[:, k // 2, k % 2, :, group * 128:(group + 1) * 128] = moved[:, k * 128:(k + 1) * 128].reshape(3, 8, 128)
    pair = [pltpu.make_async_remote_copy(src_ref=src, dst_ref=dst, send_sem=pair_send.at[k], recv_sem=pair_recv.at[k],
                                         device_id={"c": 1 - core}, device_id_type=MESH)
            for k, (src, dst) in enumerate(((perm.at[:, 1 - core], pack.at[:, 0:2, rows]),
                                            (x_ref, x_val.at[mine]), (g_ref, g_val.at[mine])))]
    for copy in pair[1:]:
        copy.start()
    pair[0].start()
    own = pltpu.make_async_copy(perm.at[:, core], pack.at[:, 0:2, rows], loc_sem.at[3])
    own.start()
    local[0].wait()
    own.wait()
    pair[0].wait_recv()
    net_a, net_b, net_c = (Sender(near, *sems) for sems in ((send_a, recv_a), (send_b, recv_b), (send_c, recv_c)))
    ring = Gather(width, me, near, net_a, buf)
    line = [Gather(width, me, near, net, lines, (k,), 2) for k, net in ((0, net_b), (1, net_c))]
    ahead = Gather(width, me, near, net_b, quarter, (), 1)
    starts = [pltpu.make_async_copy(pack.at[0], view(buf, (slice(None),), CHIPS, me), line_sem.at[0, 0])]
    for k in range(2):
        for job, (mat, cols, order) in enumerate(jobs_of(width)):
            starts.append(pltpu.make_async_copy(pack.at[1 + k, mat, :, pl.ds(*cols)], line[k].block(job, 3), line_sem.at[1 + k, job]))
    for copy in starts:
        copy.start()
    save = pltpu.make_async_copy(pack.at[0], packed_out, loc_sem.at[4])
    save.start()
    for copy in starts:
        copy.wait()
    for part in [ring] + line:
        part.send(0)
    ring.forward(0)
    ring.finish(0)
    ring.send(1)
    for part in line:
        part.forward(0)
    ring.forward(1)
    ring.finish(1)
    ring.last_sends(full_out, store_sem)
    for part in line:
        part.finish(0)
    lines_save = [pltpu.make_async_copy(lines.at[k], out, loc_sem.at[9 + k]) for k, out in enumerate((line_out_0, line_out_1))]
    for copy in lines_save:
        copy.start()
    loads = ahead.load(lines.at[0], 2, quarter_sem)
    for copy in loads:
        copy.start()
    for copy in loads:
        copy.wait()
    ahead.send(1)
    for copy in local[1:]:
        copy.wait()
    for copy in pair[1:]:
        copy.wait_recv()
    outs = [pltpu.make_async_copy(x_val, x_out, loc_sem.at[6]), pltpu.make_async_copy(g_val, g_out, loc_sem.at[7])]
    for copy in outs:
        copy.start()
    ring.forward(2)
    ahead.forward(1)
    ahead.finish(1)
    outs.append(pltpu.make_async_copy(quarter, quarter_out, loc_sem.at[8]))
    outs[-1].start()
    ring.close_out(full_out, store_sem)
    for copy in outs + [save] + lines_save:
        copy.wait()
    for copy in pair:
        copy.wait_send()
    for net in (net_a, net_b, net_c):
        net.close()


def whole_of(width):
    return (4, SIDE, SIDE, SIDE, ROWS, width)


def open_call(up, down, x_loc, g_loc, call_id):
    tokens, width = x_loc.shape
    shape = lambda *dims: jax.ShapeDtypeStruct(dims, BF16)
    whole, quarter, line = whole_of(width), (4, SIDE, SIDE, ROWS, width), (4, SIDE, ROWS, width)
    vmem = lambda *dims: pltpu.VMEM(dims, BF16)
    sems = pltpu.SemaphoreType.DMA
    anywhere = pl.BlockSpec(memory_space=pl.ANY)
    return pl.pallas_call(
        functools.partial(open_kernel, width),
        out_shape=[shape(2 * tokens, width), shape(2 * tokens, width), shape(4, ROWS, width), shape(*whole), shape(*quarter), shape(*line), shape(*line)],
        in_specs=[pl.BlockSpec(memory_space=pltpu.VMEM)] + [anywhere] * 3,
        out_specs=[anywhere] * 7,
        scratch_shapes=[vmem(3, 2, 2, 8, width), vmem(3, 4, ROWS, width), vmem(2 * tokens, width), vmem(2 * tokens, width),
                        vmem(*whole), vmem(*quarter), vmem(2, *line)] + RING_SEMS * 3
        + [sems((11,)), sems((3,)), sems((3,)), sems((3, 6)), sems((6,)), sems((6, 4))],
        compiler_params=pltpu.CompilerParams(collective_id=call_id, has_side_effects=True, vmem_limit_bytes=VMEM_LIMIT),
        name="open",
    )(up, down.reshape(3, 2, ROWS, width), x_loc, g_loc)


def dot_nn(left, right):
    return lax.dot_general(left, right, (((1,), (0,)), ((), ())), preferred_element_type=F32)


def dot_nt(left, right):
    return lax.dot_general(left, right, (((1,), (1,)), ((), ())), preferred_element_type=F32)


def dot_tn(left, right):
    return lax.dot_general(left, right, (((0,), (0,)), ((), ())), preferred_element_type=F32)


def layer_kernel(forward, width, source, ahead, pre, last_layer, *refs):
    refs = list(refs)
    take = lambda wanted: refs.pop(0) if wanted else None
    stream, weights, slope_in, act_in = take(True), take(True), take(not forward), take(not forward)
    begin, ahead_in, pre_in = take(source), take(ahead), take(pre)
    result, act_out, slope_out, grad_out = take(True), take(True), take(forward), take(not forward)
    next_out, ahead_out, pre_out = take(source), take(ahead), take(pre)
    act_low, grad_low = (refs.pop(), refs.pop()) if not forward else (None, None)
    cur, mats, act, slope, part, got, pair_send, pair_recv, loc_sem, out_sem = refs[:10]
    tokens = cur.shape[0]
    tiles = tokens // TILE
    me, near = ring_places()
    core = lax.axis_index("c")
    partner = 1 - core
    first_rows, second_rows = (pl.ds(k * 2 * width, 2 * width) for k in ((0, 1) if forward else (1, 0)))
    early = [pltpu.make_async_copy(stream, cur, loc_sem.at[0]),
             pltpu.make_async_copy(weights.at[first_rows], mats.at[first_rows], loc_sem.at[1])]
    second = pltpu.make_async_copy(weights.at[second_rows], mats.at[second_rows], loc_sem.at[2])

    def tile_rows(tile):
        return pl.ds(tile * TILE if isinstance(tile, int) else pl.multiple_of(tile * TILE, TILE), TILE)

    def slope_load(tile):
        rows = tile_rows(tile)
        return pltpu.make_async_copy(slope_in.at[rows], slope.at[rows], loc_sem.at[4 + tile])

    loads = early + [second]
    if not forward:
        low_load = pltpu.make_async_copy(act_in.at[:, pl.ds(width, width)], act_low, loc_sem.at[3])
        loads = early + [slope_load(0), second, low_load] + [slope_load(tile) for tile in range(1, tiles)]
    firsts = []
    if source:
        buf, send_sem, recv_sem, start_sem, store_sem = refs[10:15]
        net = Sender(near, send_sem, recv_sem)
        ring = Gather(width, me, near, net, buf)
        firsts = ring.load(begin, 1 if source == "quarter" else 2, start_sem)
    if ahead:
        quarter, ahead_sem = refs[15:17]
        after = Gather(width, me, near, net, quarter, (), 1)
        firsts += after.load(ahead_in, 2, ahead_sem)
    if pre:
        line, pre_sem = refs[15:17]
        before = Gather(width, me, near, net, line, (), 2)
        firsts += [pltpu.make_async_copy(pre_in.at[mat, :, pl.ds(*cols)], before.block(job, 3), pre_sem.at[job])
                   for job, (mat, cols, order) in enumerate(before.jobs)]
    for copy in firsts + loads:
        copy.start()
    enter(near, bool(source), partner)
    for copy in firsts:
        copy.wait()
    if ahead:
        after.send(1)
    if pre:
        before.send(0)
    if source == "line":
        ring.send(1)
    elif source:
        ring.last_sends(next_out, store_sem)
    for copy in early:
        copy.wait()

    def exchange(tile):
        rows = pl.ds(tile * TILE, TILE)
        return pltpu.make_async_remote_copy(
            src_ref=part.at[rows], dst_ref=got.at[rows], send_sem=pair_send.at[tile], recv_sem=pair_recv.at[tile],
            device_id={"c": partner}, device_id_type=MESH)

    def compute(tile, late=None):
        rows = tile_rows(tile)
        left = cur[rows, :]
        if not forward:
            slope_load(tile).wait()
        for block in range(2):
            for cut in range(width // WIDE):
                cols = pl.ds(block * width + cut * WIDE, WIDE)
                if forward:
                    pre = dot_nn(left, mats[block * width:(block + 1) * width, cut * WIDE:(cut + 1) * WIDE])
                    act_val, slope_val = gelu_parts(pre)
                    act[rows, cols] = act_val.astype(BF16)
                    slope[rows, cols] = slope_val
                else:
                    low = (2 + block) * width + cut * WIDE
                    d_act = dot_nt(left, mats[low:low + WIDE, :])
                    act[rows, cols] = (d_act * slope[rows, cols]).astype(BF16)
        if late is not None:
            late.wait()
        if forward:
            part[rows, :] = dot_nn(act[rows, :], mats[2 * width:, :])
        else:
            part[rows, :] = dot_nt(act[rows, :width], mats[:width, :]) + dot_nt(act[rows, width:], mats[width:2 * width, :])
        exchange(tile).start()

    def compute_tiles(low, high):
        def step(tile, _):
            compute(tile)
            return 0

        lax.fori_loop(low, high, step, 0)

    def low_slab(z, _):
        slab = width // SIDE
        val = dot_tn(act_low[:, pl.ds(pl.multiple_of(z * slab, slab), slab)], cur[...])
        grad_low[z] = val.reshape(SIDE, SIDE, ROWS, width)
        return 0

    saves = []

    def save(k, low, high):
        rows = pl.ds(low * TILE, (high - low) * TILE)
        pairs = [(act, act_out)] + ([(slope, slope_out)] if forward else [])
        for n, (src, dst) in enumerate(pairs):
            saves.append(pltpu.make_async_copy(src.at[rows], dst.at[rows], out_sem.at[2 * k + n]))
            saves[-1].start()

    head = tiles // 2 if source == "quarter" else 1
    if head == 1:
        compute(0, second)
    else:
        second.wait()
        compute_tiles(0, head)
    save(0, 0, head)
    if source == "quarter":
        ring.forward(2)
    elif source:
        ring.forward(1)
    if ahead:
        after.forward(1)
    if pre:
        before.forward(0)
    if not forward:
        low_load.wait()
        lax.fori_loop(0, SIDE, low_slab, 0)
        saves.append(pltpu.make_async_copy(grad_low, grad_out, out_sem.at[1]))
        saves[-1].start()
    if source == "line":
        ring.finish(1)
        ring.last_sends(next_out, store_sem)
    compute_tiles(head, tiles)
    save(1, head, tiles)
    if source == "line":
        ring.forward(2)
    for tile in range(tiles):
        exchange(tile).wait_recv()

    def total(rows):
        return (cur[rows, :].astype(F32) + (part[rows, :] + got[rows, :])).astype(BF16)

    if last_layer:
        for k in range(tiles // 2):
            rows = pl.ds(pl.multiple_of(core * (tokens // 2) + k * TILE, TILE), TILE)
            result[k * TILE:(k + 1) * TILE, :] = total(rows)
    else:
        for k in range(tiles):
            rows = pl.ds(k * TILE, TILE)
            result[rows, :] = total(rows)
    if ahead:
        after.finish(1)
        saves.append(pltpu.make_async_copy(quarter, ahead_out, out_sem.at[4]))
        saves[-1].start()
    if pre:
        before.finish(0)
        saves.append(pltpu.make_async_copy(line, pre_out, out_sem.at[4]))
        saves[-1].start()
    if source:
        ring.close_out(next_out, store_sem)
        net.close()
    for copy in saves:
        copy.wait()
    for tile in range(tiles):
        exchange(tile).wait_send()


def layer_call(forward, stream, full, kept, call_id, source=None, begin=None, ahead=None, pre=None, last_layer=False):
    tokens, width = stream.shape
    hidden = 2 * width
    shape = jax.ShapeDtypeStruct
    whole, quarter = whole_of(width), (4, SIDE, SIDE, ROWS, width)
    args = [stream, full.reshape(4 * width, width)] + ([] if forward else list(kept))
    args += [val for val in (begin, ahead, pre) if val is not None]
    outs = [shape((tokens // 2 if last_layer else tokens, width), BF16), shape((tokens, hidden), BF16)]
    outs += [shape((tokens, hidden), F32) if forward else shape(whole[1:], F32)]
    outs += ([shape(whole, BF16)] if source else []) + ([] if ahead is None else [shape(quarter, BF16)])
    outs += [] if pre is None else [shape(quarter[1:], BF16)]
    tiles = tokens // TILE
    sems = pltpu.SemaphoreType.DMA
    scratch = [pltpu.VMEM((tokens, width), BF16), pltpu.VMEM((4 * width, width), BF16),
               pltpu.VMEM((tokens, hidden), BF16), pltpu.VMEM((tokens, hidden), F32),
               pltpu.VMEM((tokens, width), F32), pltpu.VMEM((tokens, width), F32),
               sems((tiles,)), sems((tiles,)), sems((4 + tiles,)), sems((5,))]
    if source:
        scratch += [pltpu.VMEM(whole, BF16)] + RING_SEMS + [sems((6,)), sems((6, 4))]
    if ahead is not None:
        scratch += [pltpu.VMEM(quarter, BF16), sems((6,))]
    if pre is not None:
        scratch += [pltpu.VMEM(quarter[1:], BF16), sems((6,))]
    if not forward:
        scratch += [pltpu.VMEM(whole[1:], F32), pltpu.VMEM((tokens, width), BF16)]
    return pl.pallas_call(
        functools.partial(layer_kernel, forward, width, source, ahead is not None, pre is not None, last_layer),
        out_shape=outs,
        in_specs=[pl.BlockSpec(memory_space=pl.ANY)] * len(args),
        out_specs=[pl.BlockSpec(memory_space=pltpu.VMEM)] + [pl.BlockSpec(memory_space=pl.ANY)] * (len(outs) - 1),
        scratch_shapes=scratch,
        compiler_params=pltpu.CompilerParams(collective_id=call_id, has_side_effects=True, vmem_limit_bytes=VMEM_LIMIT),
        name="forward_layer" if forward else "backward_layer",
    )(*args)


def add_into(dst, terms, lead):
    if not lead:
        dst[...] = sum((term[...] for term in terms), dst[...])
        return

    def step(k, _):
        add_into(dst.at[k], [term.at[k] for term in terms], lead[1:])
        return 0

    lax.fori_loop(0, lead[0], step, 0)


class RingSum:
    def __init__(self, width, me, near, buf, recv, send_sem, recv_sem):
        self.me, self.near, self.buf, self.recv, self.jobs = me, near, buf, recv, jobs_of(width)
        self.net = Sender(near, send_sem, recv_sem)

    def here(self, job, phase, d, part=None):
        mat, cols, order = self.jobs[job]
        sel = {a: self.me[a] for a in order[:phase]}
        sel[order[phase]] = self.near[order[phase]][d]
        if part is not None:
            sel.update(half(order[phase + 1], part))
        return view(self.buf, (mat,), CHIPS, sel, cols)

    def there(self, job, phase, slot, part=None):
        order = self.jobs[job][2]
        left = [a for a in CHIPS if a not in order[:phase + 1]]
        return view(self.recv[3 * job + phase], (slot,), left, {} if part is None else half(order[phase + 1], part))

    def lead(self, job, phase, part=None):
        order = self.jobs[job][2]
        return [2 if part is not None and a == order[phase + 1] else SIDE for a in CHIPS if a not in order[:phase + 1]]

    def push(self, job, phase, slot, d, part, to_slot, step):
        self.net.put((job, phase, slot), self.here(job, phase, d, part), self.there(job, phase, to_slot, part),
                     self.jobs[job][2][phase], step)

    def send(self, job, phase):
        if phase == 2:
            pieces = ((0, OPPOSITE, FULL, 0, NEXT), (3, PREV, FULL, 2, PREV))
        else:
            pieces = ((0, OPPOSITE, 0, 0, NEXT), (1, OPPOSITE, 1, 0, PREV), (2, NEXT, 1, 1, NEXT), (3, PREV, 0, 2, PREV))
        for slot, d, part, to_slot, step in pieces:
            self.push(job, phase, slot, d, part, to_slot, step)

    def pass_on(self, job, phase, arrived, slot, d, part, to_slot):
        self.net.got((job, phase, arrived))
        add_into(self.here(job, phase, d, part), [self.there(job, phase, 0, part)], self.lead(job, phase, part))
        self.push(job, phase, slot, d, part, to_slot, d)

    def mid(self, job, phase):
        if phase == 2:
            self.pass_on(job, phase, 0, 2, NEXT, FULL, 1)
        else:
            self.pass_on(job, phase, 0, 4, NEXT, 0, 1)
            self.pass_on(job, phase, 1, 5, PREV, 1, 2)

    def finish(self, job, phase):
        for slot in ((2, 3) if phase == 2 else (2, 3, 4, 5)):
            self.net.got((job, phase, slot))
        add_into(self.here(job, phase, HERE), [self.there(job, phase, slot) for slot in (1, 2)], self.lead(job, phase))


def recv_blocks(width):
    blocks = []
    for mat, cols, order in jobs_of(width):
        blocks += [pltpu.VMEM((3,) + (SIDE,) * (2 - phase) + (ROWS, cols[1]), F32) for phase in range(3)]
    return blocks


def sum_kernel(width, x_ref, act_ref, d_pre_ref, g_ref, low_ref, up_out, down_out, x_val, act_val, d_pre, g_val, buf, *rest):
    send_sem, recv_sem, loc_sem, theirs, wide, pair_send, pair_recv, low_sem = rest[18:]
    me, near = ring_places()
    core = lax.axis_index("c")
    ring = RingSum(width, me, near, buf, rest[:18], send_sem, recv_sem)
    low = {}
    for d in (OPPOSITE, NEXT, PREV, HERE):
        for job in SMALL:
            mat, cols, order = ring.jobs[job]
            src = view(low_ref, (), CHIPS, {order[0]: near[order[0]][d]}, cols)
            low[job, d] = pltpu.make_async_copy(src, ring.here(job, 0, d), low_sem.at[job, d])
            low[job, d].start()
    loads = [pltpu.make_async_copy(src, dst, loc_sem.at[k]) for k, (src, dst) in enumerate(
        ((g_ref, g_val), (act_ref.at[:, pl.ds(0, width)], act_val), (x_ref, x_val), (d_pre_ref, d_pre)))]
    for copy in loads:
        copy.start()
    enter(near, True, 1 - core)

    def grad(mat):
        def slab(z, _):
            if mat < 2:
                cols = pl.ds(pl.multiple_of(z * (width // SIDE), width // SIDE), width // SIDE)
                val = dot_tn(x_val[:, cols], d_pre[:, mat * width:(mat + 1) * width])
            else:
                cols = pl.ds(pl.multiple_of(z * (width // SIDE), width // SIDE), width // SIDE)
                val = dot_tn(act_val[:, cols], g_val[...])
            buf[mat, z] = val.reshape(SIDE, SIDE, ROWS, width)
            return 0

        lax.fori_loop(0, SIDE, slab, 0)

    for job in SMALL:
        for d in (OPPOSITE, NEXT, PREV):
            low[job, d].wait()
        ring.send(job, 0)
    for copy in loads:
        copy.wait()
    for mat in (2, 0, 1):
        grad(mat)
        ring.send(LARGE[mat], 0)
        if mat == 0:
            for job in SMALL:
                ring.mid(job, 0)
    for job in LARGE:
        ring.mid(job, 0)
    for job in SMALL:
        low[job, HERE].wait()
    for phase in range(3):
        for group in (SMALL, LARGE):
            for job in group:
                ring.finish(job, phase)
                if phase < 2:
                    ring.send(job, phase + 1)
        if phase < 2:
            for group in (SMALL, LARGE):
                for job in group:
                    ring.mid(job, phase + 1)
    own = [view(buf, (mat,), CHIPS, me) for mat in range(4)]
    pair = [pltpu.make_async_remote_copy(
        src_ref=own[mat].at[pl.ds(pl.multiple_of(8 * (1 - core), 8), 8)], dst_ref=theirs.at[mat], send_sem=pair_send.at[mat],
        recv_sem=pair_recv.at[mat], device_id={"c": 1 - core}, device_id_type=MESH) for mat in range(2)]
    for copy in pair:
        copy.start()
    for mat in (2, 3):
        down_out[(mat - 2) * ROWS:(mat - 1) * ROWS, :] = own[mat][...]
    places = column_places(512, 512)
    for copy in pair:
        copy.wait_recv()
    kept = pl.ds(pl.multiple_of(8 * core, 8), 8)
    for mat in range(2):
        first, second = own[mat][kept, :], theirs[mat]
        low, high = jnp.where(core == 0, first, second), jnp.where(core == 0, second, first)
        for group in range(width // 128):
            rows, cols = slice(8 * group, 8 * group + 8), slice(128 * group, 128 * group + 128)
            wide[rows, 128 * mat:128 * mat + 128] = low[:, cols]
            wide[rows, 256 + 128 * mat:384 + 128 * mat] = high[:, cols]
    rest_val = wide[...]
    total = None
    for _ in range(3):
        piece = rest_val.astype(BF16)
        rest_val = rest_val - piece.astype(F32)
        term = dot_nt(piece, places)
        total = term if total is None else total + term
    for group in range(width // 128):
        up_out[:, 512 * group:512 * group + 512] = total[8 * group:8 * group + 8, :]
    for copy in pair:
        copy.wait_send()
    ring.net.close()


def scatter_sum(x_in, act, d_pre, g_in, low, call_id):
    tokens, width = x_in.shape
    return pl.pallas_call(
        functools.partial(sum_kernel, width),
        out_shape=[jax.ShapeDtypeStruct((8, 4 * width), F32), jax.ShapeDtypeStruct((2 * ROWS, width), F32)],
        in_specs=[pl.BlockSpec(memory_space=pl.ANY)] * 5,
        out_specs=[pl.BlockSpec(memory_space=pltpu.VMEM)] * 2,
        scratch_shapes=[pltpu.VMEM((tokens, width), BF16), pltpu.VMEM((tokens, width), BF16),
                        pltpu.VMEM((tokens, 2 * width), BF16), pltpu.VMEM((tokens, width), BF16),
                        pltpu.VMEM((4, SIDE, SIDE, SIDE, ROWS, width), F32)] + recv_blocks(width)
        + RING_SEMS + [pltpu.SemaphoreType.DMA((5,)), pltpu.VMEM((2, 8, width), F32), pltpu.VMEM((8 * (width // 128), 512), F32),
                       pltpu.SemaphoreType.DMA((2,)), pltpu.SemaphoreType.DMA((2,)), pltpu.SemaphoreType.DMA((3, 4))],
        compiler_params=pltpu.CompilerParams(collective_id=call_id, has_side_effects=True, vmem_limit_bytes=VMEM_LIMIT),
        name="scatter_sum",
    )(x_in, act, d_pre, g_in, low)


def solution(mesh):
    grid = Mesh(mesh.devices.reshape(SIDE, SIDE, SIDE, 2), ALL)
    tok_spec = P(ALL, None)
    weight_spec = P(None, ALL, None)

    def device_step(x_loc, up_loc, down_loc, g_loc):
        ids = itertools.count()
        x_0, g_3, packed, full, quarter_1, line_1, line_2 = open_call(up_loc, down_loc, x_loc, g_loc, next(ids))
        x_1, act_0, slope_0, full, quarter_2 = layer_call(True, x_0, full, None, next(ids), "quarter", quarter_1, line_2)
        x_2, act_1, slope_1, full = layer_call(True, x_1, full, None, next(ids), "quarter", quarter_2)
        y_out, act_2, slope_2, full = layer_call(True, x_2, full, None, next(ids), "line", line_2, last_layer=True)
        g_2, d_pre_2, low_2, full, line_0 = layer_call(False, g_3, full, (slope_2, act_2), next(ids), "line", line_1, pre=packed)
        sum_2 = scatter_sum(x_2, act_2, d_pre_2, g_3, low_2, next(ids))
        g_1, d_pre_1, low_1, full = layer_call(False, g_2, full, (slope_1, act_1), next(ids), "line", line_0)
        sum_1 = scatter_sum(x_1, act_1, d_pre_1, g_2, low_1, next(ids))
        grad_in, d_pre_0, low_0 = layer_call(False, g_1, full, (slope_0, act_0), next(ids), last_layer=True)
        sum_0 = scatter_sum(x_0, act_0, d_pre_0, g_1, low_0, next(ids))
        grad_up, grad_down = (jnp.stack(parts) for parts in zip(sum_0, sum_1, sum_2, strict=True))
        return y_out, grad_in, grad_up, grad_down

    return jax.shard_map(device_step, mesh=grid, in_specs=(tok_spec, weight_spec, weight_spec, tok_spec),
                         out_specs=(tok_spec, tok_spec, weight_spec, weight_spec), check_vma=False)
```

```python
import functools
import itertools
import math

import jax
import jax.numpy as jnp
from jax import lax
from jax.experimental import pallas as pl
from jax.experimental.pallas import tpu as pltpu
from jax.sharding import Mesh, PartitionSpec as P

CHIPS = ("z", "y", "x")
ALL = CHIPS + ("c",)
BF16 = jnp.bfloat16
F32 = jnp.float32
SIDE = 4
ROWS = 16
TILE = 256
WIDE = 512
INV_SQRT_2PI = (2.0 * math.pi) ** -0.5
VMEM_LIMIT = 63 * 1024 * 1024
MESH = pl.DeviceIdType.MESH
HERE, NEXT, OPPOSITE, PREV = range(4)
FULL = None
ORDERS = (("x", "y", "z"), ("y", "z", "x"), ("z", "x", "y"))


def gelu_parts(pre_act):
    norm_cdf = 0.5 * (1.0 + lax.erf(pre_act * (2.0 ** -0.5)))
    norm_pdf = jnp.exp(-0.5 * pre_act * pre_act) * INV_SQRT_2PI
    return pre_act * norm_cdf, norm_cdf + pre_act * norm_pdf


def jobs_of(width):
    tile = width // 8
    cuts = ((0, 3 * tile), (3 * tile, 3 * tile), (6 * tile, 2 * tile))
    return [(3, cuts[k], ORDERS[k]) for k in range(3)] + [(mat, (0, width), ORDERS[mat]) for mat in range(3)]


JOBS = range(6)
SMALL, LARGE = JOBS[:3], JOBS[3:]


def view(ref, lead, axes, sel, cols=None):
    mid = tuple(sel.get(a, slice(None)) for a in axes)
    last = (slice(None), pl.ds(*cols)) if cols is not None else ()
    return ref.at[lead + mid + last]


def half(axis, k):
    return {axis: pl.ds(2 * k, 2)}


def ring_places():
    me = {a: lax.axis_index(a) for a in CHIPS}
    near = {a: [lax.rem(me[a] + d, SIDE) for d in range(SIDE)] for a in CHIPS}
    return me, near


def enter(near, ring=True, partner=None):
    barrier = pltpu.get_barrier_semaphore()
    if ring:
        for axis in CHIPS:
            for d in (1, 3):
                pl.semaphore_signal(barrier, inc=1, device_id={axis: near[axis][d]}, device_id_type=MESH)
    if partner is not None:
        pl.semaphore_signal(barrier, inc=1, device_id={"c": partner}, device_id_type=MESH)
    pl.semaphore_wait(barrier, 6 * ring + (partner is not None))


class Sender:
    def __init__(self, near, send_sem, recv_sem):
        self.near, self.send_sem, self.recv_sem, self.open = near, send_sem, recv_sem, {}

    def put(self, key, src, dst, axis, step):
        copy = pltpu.make_async_remote_copy(
            src_ref=src, dst_ref=dst, send_sem=self.send_sem.at[key], recv_sem=self.recv_sem.at[key],
            device_id={axis: self.near[axis][step]}, device_id_type=MESH)
        copy.start()
        self.open[key] = copy

    def got(self, key):
        self.open[key].wait_recv()

    def close(self):
        for copy in self.open.values():
            copy.wait_send()


RING_SEMS = [pltpu.SemaphoreType.DMA((6, 3, 6)), pltpu.SemaphoreType.DMA((6, 3, 6))]


class Gather:
    def __init__(self, width, me, near, net, buf, lead=(), skip=0):
        self.me, self.near, self.net, self.buf, self.jobs = me, near, net, buf, jobs_of(width)
        self.lead, self.skip = lead, skip

    def block(self, job, fixed, more=None, ref=None, skip=None):
        mat, cols, order = self.jobs[job]
        skip = self.skip if skip is None else skip
        sel = {a: self.me[a] for a in order[:fixed]}
        sel.update(more or {})
        lead = self.lead if ref is None else ()
        return view(self.buf if ref is None else ref, lead + (mat,), [a for a in CHIPS if a not in order[:skip]], sel, cols)

    def push(self, job, phase, slot, d, part, step):
        order = self.jobs[job][2]
        axis = order[2 - phase]
        sel = {axis: self.near[axis][d]}
        if part is not None:
            sel.update(half(order[3 - phase], part))
        here = self.block(job, 2 - phase, sel)
        self.net.put((job, phase, slot), here, here, axis, step)

    def send(self, phase):
        halves = ((FULL, NEXT), (FULL, PREV)) if phase == 0 else ((0, NEXT), (1, PREV), (1, NEXT), (0, PREV))
        for job in JOBS:
            for slot, (part, step) in enumerate(halves):
                self.push(job, phase, slot, HERE, part, step)

    def forward(self, phase):
        for job in JOBS:
            self.net.got((job, phase, 0))
            if phase == 0:
                self.push(job, phase, 2, PREV, FULL, NEXT)
            else:
                self.push(job, phase, 4, PREV, 0, NEXT)
                self.net.got((job, phase, 1))
                self.push(job, phase, 5, NEXT, 1, PREV)

    def finish(self, phase):
        for job in JOBS:
            for slot in ((1, 2) if phase == 0 else (2, 3, 4, 5)):
                self.net.got((job, phase, slot))

    def load(self, src, fixed, sems):
        return [pltpu.make_async_copy(self.block(job, fixed, ref=src, skip=fixed), self.block(job, fixed), sems.at[job])
                for job in JOBS]

    def store(self, out, d, sems):
        for job in JOBS:
            axis = self.jobs[job][2][0]
            sel = {axis: self.near[axis][d]}
            copy = pltpu.make_async_copy(self.block(job, 0, sel), self.block(job, 0, sel, ref=out), sems.at[job, d])
            copy.start()
            self.stores.append(copy)

    def last_sends(self, out, sems):
        self.stores = []
        self.send(2)
        self.store(out, HERE, sems)

    def close_out(self, out, sems):
        for slots, places in (((2, 3), (NEXT, PREV)), ((4, 5), (OPPOSITE,))):
            for job in JOBS:
                for slot in slots:
                    self.net.got((job, 2, slot))
            for d in places:
                self.store(out, d, sems)
        for copy in self.stores:
            copy.wait()


def column_places(rows, cols):
    src = lax.broadcasted_iota(jnp.int32, (rows, cols), 0)
    dst = lax.broadcasted_iota(jnp.int32, (rows, cols), 1)
    want = ((dst & 127) >> 4) * 64 + (dst >> 8) * 32 + ((dst >> 7) & 1) * 16 + (dst & 15)
    return jnp.where(src == want, 1.0, 0.0).astype(BF16)


def open_kernel(width, up, down, x_ref, g_ref, x_out, g_out, packed_out, full_out, quarter_out, line_out_0, line_out_1,
                perm, pack, x_val, g_val, buf, quarter, lines, send_a, recv_a, send_b, recv_b, send_c, recv_c,
                loc_sem, pair_send, pair_recv, line_sem, quarter_sem, store_sem):
    me, near = ring_places()
    core = lax.axis_index("c")
    tokens = x_ref.shape[0]
    mine = pl.ds(pl.multiple_of(core * tokens, tokens), tokens)
    rows = pl.ds(pl.multiple_of(core * 8, 8), 8)
    local = [pltpu.make_async_copy(down, pack.at[:, 2:4], loc_sem.at[0]),
             pltpu.make_async_copy(x_ref, x_val.at[mine], loc_sem.at[1]),
             pltpu.make_async_copy(g_ref, g_val.at[mine], loc_sem.at[2])]
    for copy in local:
        copy.start()
    enter(near, True, 1 - core)
    places = column_places(512, 512)
    flat = up[...].reshape(24, 4 * width)
    for group in range(4 * width // 512):
        moved = lax.dot_general(flat[:, group * 512:(group + 1) * 512], places, (((1,), (0,)), ((), ())),
                                preferred_element_type=F32).astype(BF16)
        for k in range(4):
            perm[:, k // 2, k % 2, :, group * 128:(group + 1) * 128] = moved[:, k * 128:(k + 1) * 128].reshape(3, 8, 128)
    pair = [pltpu.make_async_remote_copy(src_ref=src, dst_ref=dst, send_sem=pair_send.at[k], recv_sem=pair_recv.at[k],
                                         device_id={"c": 1 - core}, device_id_type=MESH)
            for k, (src, dst) in enumerate(((perm.at[:, 1 - core], pack.at[:, 0:2, rows]),
                                            (x_ref, x_val.at[mine]), (g_ref, g_val.at[mine])))]
    for copy in pair[1:]:
        copy.start()
    pair[0].start()
    own = pltpu.make_async_copy(perm.at[:, core], pack.at[:, 0:2, rows], loc_sem.at[3])
    own.start()
    local[0].wait()
    own.wait()
    pair[0].wait_recv()
    net_a, net_b, net_c = (Sender(near, *sems) for sems in ((send_a, recv_a), (send_b, recv_b), (send_c, recv_c)))
    ring = Gather(width, me, near, net_a, buf)
    line = [Gather(width, me, near, net, lines, (k,), 2) for k, net in ((0, net_b), (1, net_c))]
    ahead = Gather(width, me, near, net_b, quarter, (), 1)
    starts = [pltpu.make_async_copy(pack.at[0], view(buf, (slice(None),), CHIPS, me), line_sem.at[0, 0])]
    for k in range(2):
        for job, (mat, cols, order) in enumerate(jobs_of(width)):
            starts.append(pltpu.make_async_copy(pack.at[1 + k, mat, :, pl.ds(*cols)], line[k].block(job, 3), line_sem.at[1 + k, job]))
    for copy in starts:
        copy.start()
    save = pltpu.make_async_copy(pack.at[0], packed_out, loc_sem.at[4])
    save.start()
    for copy in starts:
        copy.wait()
    for part in [ring] + line:
        part.send(0)
    ring.forward(0)
    ring.finish(0)
    ring.send(1)
    for part in line:
        part.forward(0)
    ring.forward(1)
    ring.finish(1)
    ring.last_sends(full_out, store_sem)
    for part in line:
        part.finish(0)
    lines_save = [pltpu.make_async_copy(lines.at[k], out, loc_sem.at[9 + k]) for k, out in enumerate((line_out_0, line_out_1))]
    for copy in lines_save:
        copy.start()
    loads = ahead.load(lines.at[0], 2, quarter_sem)
    for copy in loads:
        copy.start()
    for copy in loads:
        copy.wait()
    ahead.send(1)
    for copy in local[1:]:
        copy.wait()
    for copy in pair[1:]:
        copy.wait_recv()
    outs = [pltpu.make_async_copy(x_val, x_out, loc_sem.at[6]), pltpu.make_async_copy(g_val, g_out, loc_sem.at[7])]
    for copy in outs:
        copy.start()
    ring.forward(2)
    ahead.forward(1)
    ahead.finish(1)
    outs.append(pltpu.make_async_copy(quarter, quarter_out, loc_sem.at[8]))
    outs[-1].start()
    ring.close_out(full_out, store_sem)
    for copy in outs + [save] + lines_save:
        copy.wait()
    for copy in pair:
        copy.wait_send()
    for net in (net_a, net_b, net_c):
        net.close()


def whole_of(width):
    return (4, SIDE, SIDE, SIDE, ROWS, width)


def open_call(up, down, x_loc, g_loc, call_id):
    tokens, width = x_loc.shape
    shape = lambda *dims: jax.ShapeDtypeStruct(dims, BF16)
    whole, quarter, line = whole_of(width), (4, SIDE, SIDE, ROWS, width), (4, SIDE, ROWS, width)
    vmem = lambda *dims: pltpu.VMEM(dims, BF16)
    sems = pltpu.SemaphoreType.DMA
    anywhere = pl.BlockSpec(memory_space=pl.ANY)
    return pl.pallas_call(
        functools.partial(open_kernel, width),
        out_shape=[shape(2 * tokens, width), shape(2 * tokens, width), shape(4, ROWS, width), shape(*whole), shape(*quarter), shape(*line), shape(*line)],
        in_specs=[pl.BlockSpec(memory_space=pltpu.VMEM)] + [anywhere] * 3,
        out_specs=[anywhere] * 7,
        scratch_shapes=[vmem(3, 2, 2, 8, width), vmem(3, 4, ROWS, width), vmem(2 * tokens, width), vmem(2 * tokens, width),
                        vmem(*whole), vmem(*quarter), vmem(2, *line)] + RING_SEMS * 3
        + [sems((11,)), sems((3,)), sems((3,)), sems((3, 6)), sems((6,)), sems((6, 4))],
        compiler_params=pltpu.CompilerParams(collective_id=call_id, has_side_effects=True, vmem_limit_bytes=VMEM_LIMIT),
        name="open",
    )(up, down.reshape(3, 2, ROWS, width), x_loc, g_loc)


def dot_nn(left, right):
    return lax.dot_general(left, right, (((1,), (0,)), ((), ())), preferred_element_type=F32)


def dot_nt(left, right):
    return lax.dot_general(left, right, (((1,), (1,)), ((), ())), preferred_element_type=F32)


def dot_tn(left, right):
    return lax.dot_general(left, right, (((0,), (0,)), ((), ())), preferred_element_type=F32)


def layer_kernel(forward, width, source, ahead, pre, last_layer, *refs):
    refs = list(refs)
    take = lambda wanted: refs.pop(0) if wanted else None
    stream, weights, slope_in, act_in = take(True), take(True), take(not forward), take(not forward)
    begin, ahead_in, pre_in = take(source), take(ahead), take(pre)
    result, act_out, slope_out, grad_out = take(True), take(True), take(forward), take(not forward)
    next_out, ahead_out, pre_out = take(source), take(ahead), take(pre)
    act_low, grad_low = (refs.pop(), refs.pop()) if not forward else (None, None)
    cur, mats, act, slope, part, got, pair_send, pair_recv, loc_sem, out_sem = refs[:10]
    tokens = cur.shape[0]
    tiles = tokens // TILE
    me, near = ring_places()
    core = lax.axis_index("c")
    partner = 1 - core
    first_rows, second_rows = (pl.ds(k * 2 * width, 2 * width) for k in ((0, 1) if forward else (1, 0)))
    early = [pltpu.make_async_copy(stream, cur, loc_sem.at[0]),
             pltpu.make_async_copy(weights.at[first_rows], mats.at[first_rows], loc_sem.at[1])]
    second = pltpu.make_async_copy(weights.at[second_rows], mats.at[second_rows], loc_sem.at[2])

    def tile_rows(tile):
        return pl.ds(tile * TILE if isinstance(tile, int) else pl.multiple_of(tile * TILE, TILE), TILE)

    def slope_load(tile):
        rows = tile_rows(tile)
        return pltpu.make_async_copy(slope_in.at[rows], slope.at[rows], loc_sem.at[4 + tile])

    loads = early + [second]
    if not forward:
        low_load = pltpu.make_async_copy(act_in.at[:, pl.ds(width, width)], act_low, loc_sem.at[3])
        loads = early + [slope_load(0), second, low_load] + [slope_load(tile) for tile in range(1, tiles)]
    firsts = []
    if source:
        buf, send_sem, recv_sem, start_sem, store_sem = refs[10:15]
        net = Sender(near, send_sem, recv_sem)
        ring = Gather(width, me, near, net, buf)
        firsts = ring.load(begin, 1 if source == "quarter" else 2, start_sem)
    if ahead:
        quarter, ahead_sem = refs[15:17]
        after = Gather(width, me, near, net, quarter, (), 1)
        firsts += after.load(ahead_in, 2, ahead_sem)
    if pre:
        line, pre_sem = refs[15:17]
        before = Gather(width, me, near, net, line, (), 2)
        firsts += [pltpu.make_async_copy(pre_in.at[mat, :, pl.ds(*cols)], before.block(job, 3), pre_sem.at[job])
                   for job, (mat, cols, order) in enumerate(before.jobs)]
    for copy in firsts + loads:
        copy.start()
    enter(near, bool(source), partner)
    for copy in firsts:
        copy.wait()
    if ahead:
        after.send(1)
    if pre:
        before.send(0)
    if source == "line":
        ring.send(1)
    elif source:
        ring.last_sends(next_out, store_sem)
    for copy in early:
        copy.wait()

    def exchange(tile):
        rows = pl.ds(tile * TILE, TILE)
        return pltpu.make_async_remote_copy(
            src_ref=part.at[rows], dst_ref=got.at[rows], send_sem=pair_send.at[tile], recv_sem=pair_recv.at[tile],
            device_id={"c": partner}, device_id_type=MESH)

    def compute(tile, late=None):
        rows = tile_rows(tile)
        left = cur[rows, :]
        if not forward:
            slope_load(tile).wait()
        for block in range(2):
            for cut in range(width // WIDE):
                cols = pl.ds(block * width + cut * WIDE, WIDE)
                if forward:
                    pre = dot_nn(left, mats[block * width:(block + 1) * width, cut * WIDE:(cut + 1) * WIDE])
                    act_val, slope_val = gelu_parts(pre)
                    act[rows, cols] = act_val.astype(BF16)
                    slope[rows, cols] = slope_val
                else:
                    low = (2 + block) * width + cut * WIDE
                    d_act = dot_nt(left, mats[low:low + WIDE, :])
                    act[rows, cols] = (d_act * slope[rows, cols]).astype(BF16)
        if late is not None:
            late.wait()
        if forward:
            part[rows, :] = dot_nn(act[rows, :], mats[2 * width:, :])
        else:
            part[rows, :] = dot_nt(act[rows, :width], mats[:width, :]) + dot_nt(act[rows, width:], mats[width:2 * width, :])
        exchange(tile).start()

    def compute_tiles(low, high):
        def step(tile, _):
            compute(tile)
            return 0

        lax.fori_loop(low, high, step, 0)

    def low_slab(z, _):
        slab = width // SIDE
        val = dot_tn(act_low[:, pl.ds(pl.multiple_of(z * slab, slab), slab)], cur[...])
        grad_low[z] = val.reshape(SIDE, SIDE, ROWS, width)
        return 0

    saves = []

    def save(k, low, high):
        rows = pl.ds(low * TILE, (high - low) * TILE)
        pairs = [(act, act_out)] + ([(slope, slope_out)] if forward else [])
        for n, (src, dst) in enumerate(pairs):
            saves.append(pltpu.make_async_copy(src.at[rows], dst.at[rows], out_sem.at[2 * k + n]))
            saves[-1].start()

    head = tiles // 2 if source == "quarter" else 1
    if head == 1:
        compute(0, second)
    else:
        second.wait()
        compute_tiles(0, head)
    save(0, 0, head)
    if source == "quarter":
        ring.forward(2)
    elif source:
        ring.forward(1)
    if ahead:
        after.forward(1)
    if pre:
        before.forward(0)
    if not forward:
        low_load.wait()
        lax.fori_loop(0, SIDE, low_slab, 0)
        saves.append(pltpu.make_async_copy(grad_low, grad_out, out_sem.at[1]))
        saves[-1].start()
    if source == "line":
        ring.finish(1)
        ring.last_sends(next_out, store_sem)
    compute_tiles(head, tiles)
    save(1, head, tiles)
    if source == "line":
        ring.forward(2)
    for tile in range(tiles):
        exchange(tile).wait_recv()

    def total(rows):
        return (cur[rows, :].astype(F32) + (part[rows, :] + got[rows, :])).astype(BF16)

    if last_layer:
        for k in range(tiles // 2):
            rows = pl.ds(pl.multiple_of(core * (tokens // 2) + k * TILE, TILE), TILE)
            result[k * TILE:(k + 1) * TILE, :] = total(rows)
    else:
        for k in range(tiles):
            rows = pl.ds(k * TILE, TILE)
            result[rows, :] = total(rows)
    if ahead:
        after.finish(1)
        saves.append(pltpu.make_async_copy(quarter, ahead_out, out_sem.at[4]))
        saves[-1].start()
    if pre:
        before.finish(0)
        saves.append(pltpu.make_async_copy(line, pre_out, out_sem.at[4]))
        saves[-1].start()
    if source:
        ring.close_out(next_out, store_sem)
        net.close()
    for copy in saves:
        copy.wait()
    for tile in range(tiles):
        exchange(tile).wait_send()


def layer_call(forward, stream, full, kept, call_id, source=None, begin=None, ahead=None, pre=None, last_layer=False):
    tokens, width = stream.shape
    hidden = 2 * width
    shape = jax.ShapeDtypeStruct
    whole, quarter = whole_of(width), (4, SIDE, SIDE, ROWS, width)
    args = [stream, full.reshape(4 * width, width)] + ([] if forward else list(kept))
    args += [val for val in (begin, ahead, pre) if val is not None]
    outs = [shape((tokens // 2 if last_layer else tokens, width), BF16), shape((tokens, hidden), BF16)]
    outs += [shape((tokens, hidden), F32) if forward else shape(whole[1:], F32)]
    outs += ([shape(whole, BF16)] if source else []) + ([] if ahead is None else [shape(quarter, BF16)])
    outs += [] if pre is None else [shape(quarter[1:], BF16)]
    tiles = tokens // TILE
    sems = pltpu.SemaphoreType.DMA
    scratch = [pltpu.VMEM((tokens, width), BF16), pltpu.VMEM((4 * width, width), BF16),
               pltpu.VMEM((tokens, hidden), BF16), pltpu.VMEM((tokens, hidden), F32),
               pltpu.VMEM((tokens, width), F32), pltpu.VMEM((tokens, width), F32),
               sems((tiles,)), sems((tiles,)), sems((4 + tiles,)), sems((5,))]
    if source:
        scratch += [pltpu.VMEM(whole, BF16)] + RING_SEMS + [sems((6,)), sems((6, 4))]
    if ahead is not None:
        scratch += [pltpu.VMEM(quarter, BF16), sems((6,))]
    if pre is not None:
        scratch += [pltpu.VMEM(quarter[1:], BF16), sems((6,))]
    if not forward:
        scratch += [pltpu.VMEM(whole[1:], F32), pltpu.VMEM((tokens, width), BF16)]
    return pl.pallas_call(
        functools.partial(layer_kernel, forward, width, source, ahead is not None, pre is not None, last_layer),
        out_shape=outs,
        in_specs=[pl.BlockSpec(memory_space=pl.ANY)] * len(args),
        out_specs=[pl.BlockSpec(memory_space=pltpu.VMEM)] + [pl.BlockSpec(memory_space=pl.ANY)] * (len(outs) - 1),
        scratch_shapes=scratch,
        compiler_params=pltpu.CompilerParams(collective_id=call_id, has_side_effects=True, vmem_limit_bytes=VMEM_LIMIT),
        name="forward_layer" if forward else "backward_layer",
    )(*args)


def add_into(dst, terms, lead):
    if not lead:
        dst[...] = sum((term[...] for term in terms), dst[...])
        return

    def step(k, _):
        add_into(dst.at[k], [term.at[k] for term in terms], lead[1:])
        return 0

    lax.fori_loop(0, lead[0], step, 0)


class RingSum:
    def __init__(self, width, me, near, buf, recv, send_sem, recv_sem):
        self.me, self.near, self.buf, self.recv, self.jobs = me, near, buf, recv, jobs_of(width)
        self.net = Sender(near, send_sem, recv_sem)

    def here(self, job, phase, d, part=None):
        mat, cols, order = self.jobs[job]
        sel = {a: self.me[a] for a in order[:phase]}
        sel[order[phase]] = self.near[order[phase]][d]
        if part is not None:
            sel.update(half(order[phase + 1], part))
        return view(self.buf, (mat,), CHIPS, sel, cols)

    def there(self, job, phase, slot, part=None):
        order = self.jobs[job][2]
        left = [a for a in CHIPS if a not in order[:phase + 1]]
        return view(self.recv[3 * job + phase], (slot,), left, {} if part is None else half(order[phase + 1], part))

    def lead(self, job, phase, part=None):
        order = self.jobs[job][2]
        return [2 if part is not None and a == order[phase + 1] else SIDE for a in CHIPS if a not in order[:phase + 1]]

    def push(self, job, phase, slot, d, part, to_slot, step):
        self.net.put((job, phase, slot), self.here(job, phase, d, part), self.there(job, phase, to_slot, part),
                     self.jobs[job][2][phase], step)

    def send(self, job, phase):
        if phase == 2:
            pieces = ((0, OPPOSITE, FULL, 0, NEXT), (3, PREV, FULL, 2, PREV))
        else:
            pieces = ((0, OPPOSITE, 0, 0, NEXT), (1, OPPOSITE, 1, 0, PREV), (2, NEXT, 1, 1, NEXT), (3, PREV, 0, 2, PREV))
        for slot, d, part, to_slot, step in pieces:
            self.push(job, phase, slot, d, part, to_slot, step)

    def pass_on(self, job, phase, arrived, slot, d, part, to_slot):
        self.net.got((job, phase, arrived))
        add_into(self.here(job, phase, d, part), [self.there(job, phase, 0, part)], self.lead(job, phase, part))
        self.push(job, phase, slot, d, part, to_slot, d)

    def mid(self, job, phase):
        if phase == 2:
            self.pass_on(job, phase, 0, 2, NEXT, FULL, 1)
        else:
            self.pass_on(job, phase, 0, 4, NEXT, 0, 1)
            self.pass_on(job, phase, 1, 5, PREV, 1, 2)

    def finish(self, job, phase):
        for slot in ((2, 3) if phase == 2 else (2, 3, 4, 5)):
            self.net.got((job, phase, slot))
        add_into(self.here(job, phase, HERE), [self.there(job, phase, slot) for slot in (1, 2)], self.lead(job, phase))


def recv_blocks(width):
    blocks = []
    for mat, cols, order in jobs_of(width):
        blocks += [pltpu.VMEM((3,) + (SIDE,) * (2 - phase) + (ROWS, cols[1]), F32) for phase in range(3)]
    return blocks


def sum_kernel(width, x_ref, act_ref, d_pre_ref, g_ref, low_ref, up_out, down_out, x_val, act_val, d_pre, g_val, buf, *rest):
    send_sem, recv_sem, loc_sem, theirs, wide, pair_send, pair_recv, low_sem = rest[18:]
    me, near = ring_places()
    core = lax.axis_index("c")
    ring = RingSum(width, me, near, buf, rest[:18], send_sem, recv_sem)
    low = {}
    for d in (OPPOSITE, NEXT, PREV, HERE):
        for job in SMALL:
            mat, cols, order = ring.jobs[job]
            src = view(low_ref, (), CHIPS, {order[0]: near[order[0]][d]}, cols)
            low[job, d] = pltpu.make_async_copy(src, ring.here(job, 0, d), low_sem.at[job, d])
            low[job, d].start()
    loads = [pltpu.make_async_copy(src, dst, loc_sem.at[k]) for k, (src, dst) in enumerate(
        ((g_ref, g_val), (act_ref.at[:, pl.ds(0, width)], act_val), (x_ref, x_val), (d_pre_ref, d_pre)))]
    for copy in loads:
        copy.start()
    enter(near, True, 1 - core)

    def grad(mat):
        def slab(z, _):
            if mat < 2:
                cols = pl.ds(pl.multiple_of(z * (width // SIDE), width // SIDE), width // SIDE)
                val = dot_tn(x_val[:, cols], d_pre[:, mat * width:(mat + 1) * width])
            else:
                cols = pl.ds(pl.multiple_of(z * (width // SIDE), width // SIDE), width // SIDE)
                val = dot_tn(act_val[:, cols], g_val[...])
            buf[mat, z] = val.reshape(SIDE, SIDE, ROWS, width)
            return 0

        lax.fori_loop(0, SIDE, slab, 0)

    for job in SMALL:
        for d in (OPPOSITE, NEXT, PREV):
            low[job, d].wait()
        ring.send(job, 0)
    for copy in loads:
        copy.wait()
    for mat in (2, 0, 1):
        grad(mat)
        ring.send(LARGE[mat], 0)
        if mat == 0:
            for job in SMALL:
                ring.mid(job, 0)
    for job in LARGE:
        ring.mid(job, 0)
    for job in SMALL:
        low[job, HERE].wait()
    for phase in range(2):
        for job in JOBS:
            ring.finish(job, phase)
            ring.send(job, phase + 1)
        for job in JOBS:
            ring.mid(job, phase + 1)
    for job in LARGE[:2]:
        ring.finish(job, 2)
    own = [view(buf, (mat,), CHIPS, me) for mat in range(4)]
    pair = [pltpu.make_async_remote_copy(
        src_ref=own[mat].at[pl.ds(pl.multiple_of(8 * (1 - core), 8), 8)], dst_ref=theirs.at[mat], send_sem=pair_send.at[mat],
        recv_sem=pair_recv.at[mat], device_id={"c": 1 - core}, device_id_type=MESH) for mat in range(2)]
    for copy in pair:
        copy.start()
    for job in (LARGE[2], *SMALL):
        ring.finish(job, 2)
    for mat in (2, 3):
        down_out[(mat - 2) * ROWS:(mat - 1) * ROWS, :] = own[mat][...]
    places = column_places(512, 512)
    for copy in pair:
        copy.wait_recv()
    kept = pl.ds(pl.multiple_of(8 * core, 8), 8)
    for mat in range(2):
        first, second = own[mat][kept, :], theirs[mat]
        low, high = jnp.where(core == 0, first, second), jnp.where(core == 0, second, first)
        for group in range(width // 128):
            rows, cols = slice(8 * group, 8 * group + 8), slice(128 * group, 128 * group + 128)
            wide[rows, 128 * mat:128 * mat + 128] = low[:, cols]
            wide[rows, 256 + 128 * mat:384 + 128 * mat] = high[:, cols]
    rest_val = wide[...] * 0.5
    total = None
    for _ in range(3):
        piece = rest_val.astype(BF16)
        rest_val = rest_val - piece.astype(F32)
        term = dot_nt(piece, places)
        total = term if total is None else total + term
    for group in range(width // 128):
        up_out[:, 512 * group:512 * group + 512] = total[8 * group:8 * group + 8, :] * 2.0
    for copy in pair:
        copy.wait_send()
    ring.net.close()


def scatter_sum(x_in, act, d_pre, g_in, low, call_id):
    tokens, width = x_in.shape
    return pl.pallas_call(
        functools.partial(sum_kernel, width),
        out_shape=[jax.ShapeDtypeStruct((8, 4 * width), F32), jax.ShapeDtypeStruct((2 * ROWS, width), F32)],
        in_specs=[pl.BlockSpec(memory_space=pl.ANY)] * 5,
        out_specs=[pl.BlockSpec(memory_space=pltpu.VMEM)] * 2,
        scratch_shapes=[pltpu.VMEM((tokens, width), BF16), pltpu.VMEM((tokens, width), BF16),
                        pltpu.VMEM((tokens, 2 * width), BF16), pltpu.VMEM((tokens, width), BF16),
                        pltpu.VMEM((4, SIDE, SIDE, SIDE, ROWS, width), F32)] + recv_blocks(width)
        + RING_SEMS + [pltpu.SemaphoreType.DMA((5,)), pltpu.VMEM((2, 8, width), F32), pltpu.VMEM((8 * (width // 128), 512), F32),
                       pltpu.SemaphoreType.DMA((2,)), pltpu.SemaphoreType.DMA((2,)), pltpu.SemaphoreType.DMA((3, 4))],
        compiler_params=pltpu.CompilerParams(collective_id=call_id, has_side_effects=True, vmem_limit_bytes=VMEM_LIMIT),
        name="scatter_sum",
    )(x_in, act, d_pre, g_in, low)


def solution(mesh):
    grid = Mesh(mesh.devices.reshape(SIDE, SIDE, SIDE, 2), ALL)
    tok_spec = P(ALL, None)
    weight_spec = P(None, ALL, None)

    def device_step(x_loc, up_loc, down_loc, g_loc):
        ids = itertools.count()
        x_0, g_3, packed, full, quarter_1, line_1, line_2 = open_call(up_loc, down_loc, x_loc, g_loc, next(ids))
        x_1, act_0, slope_0, full, quarter_2 = layer_call(True, x_0, full, None, next(ids), "quarter", quarter_1, line_2)
        x_2, act_1, slope_1, full = layer_call(True, x_1, full, None, next(ids), "quarter", quarter_2)
        y_out, act_2, slope_2, full = layer_call(True, x_2, full, None, next(ids), "line", line_2, last_layer=True)
        g_2, d_pre_2, low_2, full, line_0 = layer_call(False, g_3, full, (slope_2, act_2), next(ids), "line", line_1, pre=packed)
        sum_2 = scatter_sum(x_2, act_2, d_pre_2, g_3, low_2, next(ids))
        g_1, d_pre_1, low_1, full = layer_call(False, g_2, full, (slope_1, act_1), next(ids), "line", line_0)
        sum_1 = scatter_sum(x_1, act_1, d_pre_1, g_2, low_1, next(ids))
        grad_in, d_pre_0, low_0 = layer_call(False, g_1, full, (slope_0, act_0), next(ids), last_layer=True)
        sum_0 = scatter_sum(x_0, act_0, d_pre_0, g_1, low_0, next(ids))
        grad_up, grad_down = (jnp.stack(parts) for parts in zip(sum_0, sum_1, sum_2, strict=True))
        return y_out, grad_in, grad_up, grad_down

    return jax.shard_map(device_step, mesh=grid, in_specs=(tok_spec, weight_spec, weight_spec, tok_spec),
                         out_specs=(tok_spec, tok_spec, weight_spec, weight_spec), check_vma=False)
```
